256 devices in a mesh: dp: 32 (over z_lo, x, core), cls: 8 (over y, z_hi).
Axes of the slice: x: 4, y: 4, z: 8 (z_hi: 2, z_lo: 4; z = z_hi * 4 + z_lo), core: 2. Of those that a mesh axis runs over, the one named last changes fastest.
Arguments:
- features: bfloat16 [512, 131072], P('cls', 'dp'), may hold values from -200 to 200
- labels: int32 [131072], P('dp'), may hold values from 0 to 7
- coeffs: bfloat16 [8, 512], P('cls'), may hold values from -0.176776695 to 0.176776695
- smoothing: float32 [8], replicated, may hold values from 0.1 to 1
- pair_slots: int32 [40], P('cls'), may hold values from 0 to 39, each once
Outputs:
- hessian: float32 [512, 40, 512], P('dp', 'cls')
- gradient: float32 [8, 512], P('cls', 'dp')
The draws below stay inside these ranges and needn't reach their ends.
Inputs may be any that keep to these rules, and one draw needn't show every extreme that they name: `pair_slots`: the entry of slot s of the index c of cls is entry c * 5 + s; an entry below 36 names that pair block, a larger entry marks an empty slot; every value appears once.
All inputs are finite; a program needn't handle non-finite values.
Results may differ from the reference program's by a relative error of at most 0.0003.
Values may be sent and summed in bfloat16 or wider, within the bound.
A program may use at most 128 MiB of HBM per device.

```python
import math
import jax
import jax.numpy as jnp
import numpy as np
from jax import lax

CLASSES = 8
BASIS = 512
ROWS_DEV = 4096
ROWS = 131072
PAIRS = 36
SLOTS = 5
N_CLS = 8


def coeff_table(key):
    values = jax.random.truncated_normal(jax.random.fold_in(key, 11), -4.0, 4.0, (CLASSES, BASIS), jnp.float32)
    return values / math.sqrt(BASIS)


def draw_coeffs(key, part):
    return coeff_table(key).astype(jnp.bfloat16)


def draw_features(key, part):
    values = jax.random.truncated_normal(jax.random.fold_in(key, 12), -6.0, 6.0, (ROWS, BASIS), jnp.float32)
    return jnp.clip(values, -200.0, 200.0).T.astype(jnp.bfloat16)


def place_ends(entries, key, low, top_value):
    spot = [jax.random.randint(jax.random.fold_in(key, axis), (), 0, length) for axis, length in enumerate(entries.shape)]
    widest = entries.shape.index(max(entries.shape))
    beside = spot[:widest] + [(spot[widest] + 1) % entries.shape[widest]] + spot[widest + 1:]
    return entries.at[tuple(spot)].set(low).at[tuple(beside)].set(top_value)


def setup_inputs(seed: int = 0) -> dict:
    seeds = jax.random.split(jax.random.key(seed), 6)
    features = draw_features(jax.random.fold_in(seeds[5], 71), 0)
    labels = place_ends(jax.random.randint(seeds[1], (ROWS,), 0, CLASSES), jax.random.fold_in(seeds[1], 1), 0, CLASSES - 1).astype(jnp.int32)
    coeffs = draw_coeffs(jax.random.fold_in(seeds[5], 71), 0)
    smoothing = jnp.clip(jnp.exp(jax.random.uniform(seeds[3], (CLASSES,), jnp.float32, math.log(0.1), math.log(1.0))), 0.1, 1.0)
    pair_slots = jax.random.permutation(seeds[4], N_CLS * SLOTS).astype(jnp.int32)
    return dict(features=features, labels=labels, coeffs=coeffs, smoothing=smoothing, pair_slots=pair_slots)


def pair_tables():
    first_list = []
    second_list = []
    for class_one in range(CLASSES):
        for class_two in range(class_one, CLASSES):
            first_list.append(class_one)
            second_list.append(class_two)
    return np.array(first_list, np.int32), np.array(second_list, np.int32)


def second_differences(width):
    index_row = jnp.arange(width - 2)[:, None]
    index_col = jnp.arange(width)[None, :]
    return ((index_col == index_row).astype(jnp.float32) - 2.0 * (index_col == index_row + 1).astype(jnp.float32)
            + (index_col == index_row + 2).astype(jnp.float32))


def reference(features, labels, coeffs, smoothing, pair_slots):
    matrix = features.T
    scores = jnp.dot(matrix, coeffs.T, preferred_element_type=jnp.float32)
    row_top = jnp.max(scores, axis=1, keepdims=True)
    exponent = jnp.exp(scores - row_top)
    probs = exponent / jnp.sum(exponent, axis=1, keepdims=True)
    differences = second_differences(BASIS)
    penalty_matrix = jnp.dot(differences.T, differences, precision=lax.Precision.HIGHEST,
                             preferred_element_type=jnp.float32)
    first_tab, second_tab = pair_tables()
    first_tab = jnp.asarray(first_tab)
    second_tab = jnp.asarray(second_tab)
    row_weight = 1.0 / ROWS_DEV

    def pair_block(pair_number):
        class_one = first_tab[pair_number]
        class_two = second_tab[pair_number]
        same_class = (class_one == class_two).astype(jnp.float32)
        prob_one = jnp.take(probs, class_one, axis=1)
        prob_two = jnp.take(probs, class_two, axis=1)
        weights = prob_one * (same_class - prob_two)
        scaled = (matrix * weights[:, None]).astype(jnp.bfloat16)
        products = jnp.dot(scaled.T, matrix, preferred_element_type=jnp.float32) * row_weight
        return products + same_class * smoothing[class_one] * penalty_matrix

    blocks = lax.map(pair_block, jnp.arange(PAIRS, dtype=jnp.int32))
    live_slot = (pair_slots < PAIRS).astype(jnp.float32)
    pair_index = jnp.minimum(pair_slots, PAIRS - 1).astype(jnp.int32)
    chosen = blocks[pair_index] * live_slot[:, None, None]
    hessian = jnp.transpose(chosen, (1, 0, 2))
    one_hot = (labels[:, None] == jnp.arange(CLASSES, dtype=jnp.int32)[None, :]).astype(jnp.float32)
    resid = (one_hot - probs).astype(jnp.bfloat16)
    data_part = jnp.dot(resid.T, matrix, preferred_element_type=jnp.float32) * row_weight
    penalty_part = jnp.dot(coeffs.astype(jnp.float32), penalty_matrix, precision=lax.Precision.HIGHEST,
                           preferred_element_type=jnp.float32)
    gradient = data_part - smoothing[:, None] * penalty_part
    return hessian, gradient
```

```python
import jax
import jax.numpy as jnp
from jax import lax
from jax.experimental import pallas as pl
from jax.experimental.pallas import tpu as pltpu
from jax.sharding import Mesh
from jax.sharding import PartitionSpec as P

CLASSES = 8
PAIRS = CLASSES * (CLASSES + 1) // 2
STARTS = (8, 15, 21, 26, 30, 33, 35)
DIAGONAL = (0, 8, 15, 21, 26, 30, 33, 35)
AXES = ("zl", "x", "core", "y", "zh")
DP = ("zl", "x", "core")
CLS = ("y", "zh")
MESH = pl.DeviceIdType.MESH
STEPS = 8
LEVELS = 32767.0
F32 = jnp.float32
BF16 = jnp.bfloat16


def place():
    return {name: lax.axis_index(name) for name in AXES}


def remote(src, dst, send, recv, device):
    return pltpu.make_async_remote_copy(
        src_ref=src, dst_ref=dst, send_sem=send, recv_sem=recv, device_id=device, device_id_type=MESH
    )


def greet(devices):
    barrier = pltpu.get_barrier_semaphore()
    for device in devices:
        pl.semaphore_signal(barrier, inc=1, device_id=device, device_id_type=MESH)
    return barrier, len(devices)


def pair_weights(slots, probs):
    pair = jnp.minimum(slots, PAIRS - 1)
    first = jnp.zeros_like(pair)
    start = jnp.zeros_like(pair)
    for before, at in zip((0,) + STARTS, STARTS):
        later = pair >= at
        first += jnp.where(later, 1, 0)
        start += jnp.where(later, at - before, 0)
    second = pair - start + first
    live = (slots < PAIRS)[:, :1]
    first, second = first[:, :1], second[:, :1]
    prob_first = jnp.zeros_like(probs)
    prob_second = jnp.zeros_like(probs)
    for k in range(CLASSES):
        row = probs[k : k + 1, :]
        prob_first += jnp.where(first == k, row, 0.0)
        prob_second += jnp.where(second == k, row, 0.0)
    same = jnp.where(first == second, 1.0, 0.0)
    return jnp.where(live, prob_first * (same - prob_second), 0.0)


def gather_kernel(
    feat, coeffs, labels, slots,
    part_out, scale_out, grad_out,
    held, total, labs, pairs, tiles, matrix, gsum, lhs,
    own_sem, z_send, z_recv, yo_send, yo_recv, yz_send, yz_recv, op_send, op_recv,
    d_send, d_recv, t_send, t_recv, p_sem, l_sem,
):
    at = place()
    k, y, h = at["core"], at["y"], at["zh"]
    cls = y * 2 + h
    width = held.shape[2]
    half = width // 2
    rows = feat.shape[0]
    kept = feat.shape[1] // 2
    up, down, across = lax.rem(y + 1, 4), lax.rem(y + 3, 4), lax.rem(y + 2, 4)
    antipode, partner = {"zh": 1 - h}, {"core": 1 - k}

    def other(j):
        c = lax.rem(cls + j, 8)
        return c, {"y": c // 2, "zh": lax.rem(c, 2)}

    barrier, count = greet([other(j)[1] for j in range(1, 8)] + [partner])

    lanes = pl.ds(pl.multiple_of(k * half, half), half)

    def band(q, first, size):
        return held.at[q, pl.ds(pl.multiple_of(first, 64), size), lanes]

    def columns(side, q):
        return feat.at[:, pl.ds(pl.multiple_of(side * kept + q * half, half), half)]

    def own_copy(q):
        return pltpu.make_async_copy(columns(h, q), band(q, cls * rows, rows), own_sem.at[q])

    for q in range(STEPS):
        own_copy(q).start()
    label_rows = kept // 128
    own_labels = labels.at[pl.ds(pl.multiple_of(h * label_rows, 8), label_rows)]
    label_copy = pltpu.make_async_copy(own_labels, labs.at[k], l_sem.at[0])
    label_copy.start()

    row8 = lax.broadcasted_iota(jnp.int32, (8, 128), 0)
    mine = jnp.full((8, 128), 40, jnp.int32)
    for s in range(5):
        mine = jnp.where(row8 == s, slots[s], mine)
    pairs[h] = mine
    coeff_rows = coeffs[...].astype(F32)
    pieces = [coeff_rows[:, 128 * j : 128 * (j + 1)] for j in range(4)]
    tiles[cls] = jnp.concatenate(pieces + [jnp.zeros((4, 128), F32)], axis=0)

    total[...] = jnp.zeros_like(total)
    gsum[...] = jnp.zeros_like(gsum)

    pl.semaphore_wait(barrier, count)

    def z_copy(q, c):
        return remote(columns(1 - h, q), band(q, c * rows, rows), z_send.at[q], z_recv.at[q], antipode)

    def yo_copy(q, d, c):
        to = {"y": (up, down)[d]}
        return remote(columns(h, q), band(q, c * rows, rows), yo_send.at[d, q], yo_recv.at[d, q], to)

    def yz_copy(q, d, c):
        to = {"y": (up, down)[d]}
        block = band(q, c * rows, rows)
        return remote(block, block, yz_send.at[d, q], yz_recv.at[d, q], to)

    def op_copy(q, source):
        to = {"y": jnp.where(lax.rem(q, 2) == 0, up, down)}
        block = band(q, source * 2 * rows, 2 * rows)
        return remote(block, block, op_send.at[q], op_recv.at[q], to)

    def d_copy(q, i, source, lane_core):
        wide = pl.ds(pl.multiple_of(lane_core * half, half), half)
        block = held.at[q, pl.ds(pl.multiple_of(source * 2 * rows, 2 * rows), 2 * rows), wide]
        return remote(block, block, d_send.at[i, q], d_recv.at[i, q], partner)

    def tile_copy(j, c):
        _, to = other(j)
        return remote(tiles.at[c], tiles.at[c], t_send.at[j], t_recv.at[8 - j], to)

    def pair_copy(side):
        return remote(pairs.at[side], pairs.at[side], p_sem.at[0], p_sem.at[1], antipode)

    def label_send(core):
        return remote(labs.at[core], labs.at[core], l_sem.at[1], l_sem.at[2], partner)

    for j in range(1, 8):
        tile_copy(j, cls).start()
    pair_copy(h).start()
    for q in range(STEPS):
        z_copy(q, cls).start()
        for d in range(2):
            yo_copy(q, d, cls).start()
    label_copy.wait()
    label_send(k).start()

    for j in range(1, 8):
        c, _ = other(8 - j)
        tile_copy(8 - j, c).wait_recv()
    pair_copy(1 - h).wait_recv()
    label_send(1 - k).wait_recv()
    for c in range(CLASSES):
        tile = tiles[c]
        matrix[c : c + 1, :] = jnp.concatenate([tile[j : j + 1, :] for j in range(4)], axis=1)

    def stage_a(q):
        own_copy(q).wait()
        z_copy(q, y * 2 + 1 - h).wait_recv()
        for d in range(2):
            yz_copy(q, d, y * 2 + 1 - h).start()
        d_copy(q, 0, y, k).start()

    def stage_b(q):
        for d, source in ((0, down), (1, up)):
            yo_copy(q, d, source * 2 + h).wait_recv()
            yz_copy(q, d, source * 2 + 1 - h).wait_recv()
        op_copy(q, jnp.where(lax.rem(q, 2) == 0, down, up)).start()
        d_copy(q, 1, down, k).start()
        d_copy(q, 2, up, k).start()

    def stage_c(q):
        op_copy(q, across).wait_recv()
        d_copy(q, 3, across, k).start()

    def stage_d(q):
        for i, source in enumerate((y, down, up, across)):
            d_copy(q, i, source, 1 - k).wait_recv()
        block = held[q]
        scores = jnp.dot(matrix[...].astype(BF16), block, preferred_element_type=F32)
        exponent = jnp.exp(scores - jnp.max(scores, axis=0, keepdims=True))
        probs = exponent / jnp.sum(exponent, axis=0, keepdims=True)
        weights = pair_weights(pairs[k], probs)
        lab_rows = [labs[core, pl.ds(q * (half // 128) + i, 1), :] for core in range(2) for i in range(half // 128)]
        lab = jnp.concatenate(lab_rows, axis=1)
        one_hot = lax.broadcasted_iota(jnp.int32, (8, width), 0) == lab
        resid = (jnp.where(one_hot, 1.0, 0.0) - probs).astype(BF16)
        contract = (((1,), (1,)), ((), ()))
        gsum[...] += lax.dot_general(resid, block, contract, preferred_element_type=F32)
        wide = block.astype(F32)
        for s in range(5):
            lhs[s % 2] = (wide * weights[s : s + 1, :]).astype(BF16)
            total[s] += lax.dot_general(lhs[s % 2], block, contract, preferred_element_type=F32)

    def step(t, carry):
        @pl.when(t < STEPS)
        def _():
            stage_a(t)

        @pl.when((t >= 1) & (t < STEPS + 1))
        def _():
            stage_b(t - 1)

        @pl.when((t >= 2) & (t < STEPS + 2))
        def _():
            stage_c(t - 2)

        @pl.when(t >= 3)
        def _():
            stage_d(t - 3)

        return carry

    lax.fori_loop(0, STEPS + 3, step, 0)

    scales = jnp.zeros((8, 128), F32)
    for s in range(5):
        block = total[s]
        largest = jnp.max(jnp.max(jnp.abs(block), axis=0, keepdims=True), axis=1, keepdims=True)
        largest = jnp.maximum(largest, 1e-30)
        scales = jnp.where(row8 == s, largest * (1.0 / LEVELS), scales)
        coded = jnp.round(block * (LEVELS / largest)).astype(jnp.int32).astype(jnp.int16)
        for i in range(4):
            for x in range(4):
                first = i * 128 + x * 32
                part_out[x, s, 32 * i : 32 * (i + 1), :] = coded[first : first + 32, :]
    scale_out[...] = scales
    grad_out[...] = gsum[...]

    for j in range(1, 8):
        tile_copy(j, cls).wait_send()
    pair_copy(h).wait_send()
    label_send(k).wait_send()

    def drain(q, carry):
        z_copy(q, cls).wait_send()
        for d in range(2):
            yo_copy(q, d, cls).wait_send()
            yz_copy(q, d, y * 2 + 1 - h).wait_send()
        op_copy(q, across).wait_send()
        for i, source in enumerate((y, down, up, across)):
            d_copy(q, i, source, k).wait_send()
        return carry

    lax.fori_loop(0, STEPS, drain, 0)


def reduce_kernel(
    part, scales, grad, coeffs, slots, smoothing,
    hess_out, grad_out,
    got, got_scale, got_grad, sums, coded, small, far, far_small, pen_row, stage,
    x_send, x_recv, xs_send, xs_recv, xg_send, xg_recv, z_send, z_recv, zs_send, zs_recv, c_sem,
):
    at = place()
    k, x, y, h, zl = at["core"], at["x"], at["y"], at["zh"], at["zl"]
    z = h * 4 + zl

    def near(j):
        return {"x": lax.rem(x + j, 4)}

    def owner(i, e):
        return {"zl": lax.rem(zl + i, 4), "zh": k, "core": lax.rem(k + e, 2)}

    others = [near(j) for j in range(1, 4)]
    for a in range(2):
        for i in range(4):
            for e in range(2):
                if a or i or e:
                    others.append({"zl": lax.rem(zl + i, 4), "zh": lax.rem(h + a, 2), "core": lax.rem(k + e, 2)})
    barrier, count = greet(others)

    row0 = zl * 128 + x * 32 + k * 16
    ia = lax.broadcasted_iota(jnp.int32, (16, 512), 0) + row0
    ib = lax.broadcasted_iota(jnp.int32, (16, 512), 1)
    pen = jnp.zeros((16, 512), F32)
    taps = (1.0, -2.0, 1.0)
    for m in range(3):
        inside = (ia - m >= 0) & (ia - m <= 509)
        for n in range(3):
            pen += jnp.where(inside & (ib - n == ia - m), taps[m] * taps[n], 0.0)
    lane = lax.broadcasted_iota(jnp.int32, (8, 512), 1)
    row = jnp.broadcast_to(coeffs[...].astype(F32), (8, 512))
    diff = row - 2.0 * pltpu.roll(row, 511, 1) + pltpu.roll(row, 510, 1)
    diff = jnp.where(lane < 510, diff, 0.0)
    pen_row[...] = diff - 2.0 * pltpu.roll(diff, 1, 1) + pltpu.roll(diff, 2, 1)

    pl.semaphore_wait(barrier, count)

    def x_copy(s, j, source):
        to = lax.rem(x + j, 4)
        return remote(part.at[to, s], got.at[source, s], x_send.at[j, s], x_recv.at[4 - j, s], near(j))

    def xs_copy(j, source):
        return remote(scales, got_scale.at[source], xs_send.at[j], xs_recv.at[4 - j], near(j))

    def xg_copy(j, source):
        return remote(grad, got_grad.at[source], xg_send.at[j], xg_recv.at[4 - j], near(j))

    for j in (1, 3, 2):
        xs_copy(j, x).start()
    for s in range(5):
        for j in (1, 3, 2):
            x_copy(s, j, x).start()
    for j in (1, 3, 2):
        xg_copy(j, x).start()
    own_scale = pltpu.make_async_copy(scales, got_scale.at[x], c_sem.at[0])
    own_grad = pltpu.make_async_copy(grad, got_grad.at[x], c_sem.at[1])
    own_scale.start()
    own_grad.start()

    def own_part(s):
        return pltpu.make_async_copy(part.at[x, s], got.at[x, s], c_sem.at[2 + s])

    for s in range(5):
        own_part(s).start()
    own_scale.wait()
    own_grad.wait()
    for j in (1, 3, 2):
        xs_copy(4 - j, lax.rem(x + 4 - j, 4)).wait_recv()

    def z_copy(s, i, e, source):
        to = lax.rem(zl + i, 4)
        src = coded.at[s, to, lax.rem(k + e, 2)]
        return remote(src, far.at[source, s], z_send.at[i, e, s], z_recv.at[source, s], owner(i, e))

    def zs_copy(i, e, source):
        to = lax.rem(zl + i, 4)
        return remote(small.at[to], far_small.at[source], zs_send.at[i, e], zs_recv.at[source], owner(i, e))

    def to_owners(act):
        for i in (2, 1, 3, 0):
            for e in range(2):
                if i or e:
                    act(i, e)
                else:
                    pl.when(h != k)(lambda: act(0, 0))

    def own_far(s):
        return pltpu.make_async_copy(coded.at[s, zl, k], far.at[z, s], c_sem.at[8 + s])

    own_small = pltpu.make_async_copy(small.at[zl], far_small.at[z], c_sem.at[7])

    row8 = lax.broadcasted_iota(jnp.int32, (8, 128), 0)
    scale2 = jnp.zeros((8, 128), F32)
    for s in range(5):
        own_part(s).wait()
        for j in (1, 3, 2):
            x_copy(s, 4 - j, lax.rem(x + 4 - j, 4)).wait_recv()
        value = jnp.zeros((128, 512), F32)
        for source in range(4):
            scale = got_scale[source, s : s + 1, 0:1]
            value += got[source, s].astype(jnp.int32).astype(F32) * scale
        largest = jnp.max(jnp.max(jnp.abs(value), axis=0, keepdims=True), axis=1, keepdims=True)
        largest = jnp.maximum(largest, 1e-30)
        scale2 = jnp.where(row8 == s, largest * (1.0 / LEVELS), scale2)
        out = jnp.round(value * (LEVELS / largest)).astype(jnp.int32).astype(jnp.int16)
        for i in range(4):
            for e in range(2):
                first = i * 32 + e * 16
                coded[s, i, e] = out[first : first + 16, :]
        to_owners(lambda i, e: z_copy(s, i, e, z).start())
        pl.when(h == k)(lambda: own_far(s).start())

    for j in (1, 3, 2):
        xg_copy(4 - j, lax.rem(x + 4 - j, 4)).wait_recv()
    all_grad = got_grad[0] + got_grad[1] + got_grad[2] + got_grad[3]
    for i in range(4):
        small[i, 0] = all_grad[:, 128 * i : 128 * (i + 1)]
        small[i, 1] = scale2
    to_owners(lambda i, e: zs_copy(i, e, z).start())
    pl.when(h == k)(lambda: own_small.start())

    def arrived(source, wait):
        def other():
            wait(source)

        pl.when((z != source) | (h != k))(other)

    for source in range(8):
        arrived(source, lambda source: zs_copy(1, 0, source).wait_recv())
    pl.when(h == k)(lambda: own_small.wait())
    grads = far_small[0, 0]
    for source in range(1, 8):
        grads += far_small[source, 0]
    for s in range(5):
        for source in range(8):
            arrived(source, lambda source: z_copy(s, 1, 0, source).wait_recv())
        pl.when(h == k)(lambda: own_far(s).wait())
        value = jnp.zeros((16, 512), F32)
        for source in range(8):
            scale = far_small[source, 1, s : s + 1, 0:1]
            value += far[source, s].astype(jnp.int32).astype(F32) * scale
        smooth = jnp.float32(0.0)
        for j, number in enumerate(DIAGONAL):
            smooth += jnp.where(slots[s] == number, smoothing[j], 0.0)
        hess_out[s] = value * (1.0 / 4096.0) + pen * smooth

    cls = y * 2 + h
    picked = jnp.sum(jnp.where(row8 == cls, grads, 0.0), axis=0, keepdims=True) * (1.0 / 4096.0)
    pen_part = pen_row[:, pl.ds(pl.multiple_of(zl * 128, 128), 128)]
    final = picked - smoothing[cls] * pen_part
    stage[...] = pltpu.roll(final, lax.rem(128 - (x * 32 + k * 16), 128), 1)
    grad_out[...] = stage[0:1, 0:16]

    for j in (1, 3, 2):
        xs_copy(j, x).wait_send()
        xg_copy(j, x).wait_send()
        for s in range(5):
            x_copy(s, j, x).wait_send()
    to_owners(lambda i, e: zs_copy(i, e, z).wait_send())
    for s in range(5):
        to_owners(lambda i, e: z_copy(s, i, e, z).wait_send())


def local(features, labels, coeffs, smoothing, pair_slots):
    vmem = pl.BlockSpec(memory_space=pltpu.VMEM)
    smem = pl.BlockSpec(memory_space=pltpu.SMEM)
    anyspace = pl.BlockSpec(memory_space=pl.ANY)
    dma = pltpu.SemaphoreType.DMA
    half = features.shape[1] // 2 // STEPS
    part, scales, grad = pl.pallas_call(
        gather_kernel,
        out_shape=(
            jax.ShapeDtypeStruct((4, 5, 128, 512), jnp.int16),
            jax.ShapeDtypeStruct((8, 128), F32),
            jax.ShapeDtypeStruct((8, 512), F32),
        ),
        in_specs=[anyspace, vmem, anyspace, smem],
        out_specs=(vmem, vmem, vmem),
        scratch_shapes=[
            pltpu.VMEM((STEPS, 512, 2 * half), BF16),
            pltpu.VMEM((5, 512, 512), F32),
            pltpu.VMEM((2, 16, 128), jnp.int32),
            pltpu.VMEM((2, 8, 128), jnp.int32),
            pltpu.VMEM((8, 8, 128), F32),
            pltpu.VMEM((8, 512), F32),
            pltpu.VMEM((8, 512), F32),
            pltpu.VMEM((2, 512, 2 * half), BF16),
            dma((STEPS,)), dma((STEPS,)), dma((STEPS,)),
            dma((2, STEPS)), dma((2, STEPS)), dma((2, STEPS)), dma((2, STEPS)),
            dma((STEPS,)), dma((STEPS,)),
            dma((4, STEPS)), dma((4, STEPS)),
            dma((8,)), dma((8,)), dma((2,)), dma((3,)),
        ],
        compiler_params=pltpu.CompilerParams(collective_id=0, has_side_effects=True),
        name="gather",
    )(features, coeffs, labels.reshape(32, 128), pair_slots)
    hessian, gradient = pl.pallas_call(
        reduce_kernel,
        out_shape=(
            jax.ShapeDtypeStruct((5, 16, 512), F32),
            jax.ShapeDtypeStruct((1, 16), F32),
        ),
        in_specs=[anyspace, anyspace, anyspace, vmem, smem, smem],
        out_specs=(vmem, vmem),
        scratch_shapes=[
            pltpu.VMEM((4, 5, 128, 512), jnp.int16),
            pltpu.VMEM((4, 8, 128), F32),
            pltpu.VMEM((4, 8, 512), F32),
            pltpu.VMEM((8, 128), F32),
            pltpu.VMEM((5, 4, 2, 16, 512), jnp.int16),
            pltpu.VMEM((4, 2, 8, 128), F32),
            pltpu.VMEM((8, 5, 16, 512), jnp.int16),
            pltpu.VMEM((8, 2, 8, 128), F32),
            pltpu.VMEM((8, 512), F32),
            pltpu.VMEM((8, 128), F32),
            dma((4, 5)), dma((4, 5)), dma((4,)), dma((4,)), dma((4,)), dma((4,)),
            dma((4, 2, 5)), dma((8, 5)), dma((4, 2)), dma((8,)), dma((13,)),
        ],
        compiler_params=pltpu.CompilerParams(collective_id=1, has_side_effects=True),
        name="reduce",
    )(part, scales, grad, coeffs, pair_slots, smoothing)
    return hessian.transpose(1, 0, 2), gradient


def solution(mesh):
    finer = Mesh(mesh.devices.reshape(4, 4, 2, 4, 2), AXES)
    placed = (P(CLS, DP), P(DP), P(CLS, None), P(), P(CLS))
    return jax.shard_map(
        local,
        mesh=finer,
        in_specs=placed,
        out_specs=(P(DP, CLS, None), P(CLS, DP)),
        check_vma=False,
    )
```

```python
import jax
import jax.numpy as jnp
from jax import lax
from jax.experimental import pallas as pl
from jax.experimental.pallas import tpu as pltpu
from jax.sharding import Mesh
from jax.sharding import PartitionSpec as P

CLASSES = 8
PAIRS = CLASSES * (CLASSES + 1) // 2
STARTS = (8, 15, 21, 26, 30, 33, 35)
DIAGONAL = (0, 8, 15, 21, 26, 30, 33, 35)
AXES = ("zl", "x", "core", "y", "zh")
DP = ("zl", "x", "core")
CLS = ("y", "zh")
MESH = pl.DeviceIdType.MESH
STEPS = 8
LEVELS = 32767.0
F32 = jnp.float32
BF16 = jnp.bfloat16


def place():
    return {name: lax.axis_index(name) for name in AXES}


def remote(src, dst, send, recv, device):
    return pltpu.make_async_remote_copy(
        src_ref=src, dst_ref=dst, send_sem=send, recv_sem=recv, device_id=device, device_id_type=MESH
    )


def pair_weights(slots, probs):
    pair = jnp.minimum(slots, PAIRS - 1)
    first = jnp.zeros_like(pair)
    start = jnp.zeros_like(pair)
    for before, at in zip((0,) + STARTS, STARTS):
        later = pair >= at
        first += jnp.where(later, 1, 0)
        start += jnp.where(later, at - before, 0)
    second = pair - start + first
    live = (slots < PAIRS)[:, :1]
    first, second = first[:, :1], second[:, :1]
    prob_first = jnp.zeros_like(probs)
    prob_second = jnp.zeros_like(probs)
    for k in range(CLASSES):
        row = probs[k : k + 1, :]
        prob_first += jnp.where(first == k, row, 0.0)
        prob_second += jnp.where(second == k, row, 0.0)
    same = jnp.where(first == second, 1.0, 0.0)
    return jnp.where(live, prob_first * (same - prob_second), 0.0)


def newton_kernel(
    feat, coeffs, labels, slots, smoothing,
    hess_out, grad_out,
    held, sent, total, labs, pairs, tiles, matrix, gsum, scales,
    relay_q, direct_q, joint_q, got_relay, got_direct, got_joint, grads,
    coded, small, far, far_small, pen_row, stage,
    own_sem, away_sem, z_send, z_recv, yo_send, yz_send, y_recv, op_send, op_recv, d_send, d_recv,
    tz_sem, ty_send, ty_recv, p_sem, l_sem, s_send, s_recv, q_send, relay_recv, direct_recv, joint_recv,
    g_send, g_recv, f_send, f_recv, fs_send, fs_recv,
):
    at = place()
    k, x, y, h, zl = at["core"], at["x"], at["y"], at["zh"], at["zl"]
    z = h * 4 + zl
    cls = y * 2 + h
    half = held.shape[3]
    rows = feat.shape[0]
    kept = feat.shape[1] // 2
    up, down, across = lax.rem(y + 1, 4), lax.rem(y + 3, 4), lax.rem(y + 2, 4)
    antipode, partner = {"zh": 1 - h}, {"core": 1 - k}

    peers = [{"x": lax.rem(x + j, 4)} for j in range(1, 4)] + [{"y": lax.rem(y + j, 4)} for j in range(1, 4)]
    for a in range(2):
        for i in range(4):
            for e in range(2):
                if a or i or e:
                    peers.append({"zl": lax.rem(zl + i, 4), "zh": lax.rem(h + a, 2), "core": lax.rem(k + e, 2)})
    barrier = pltpu.get_barrier_semaphore()
    for device in peers[::-1]:
        pl.semaphore_signal(barrier, inc=1, device_id=device, device_id_type=MESH)

    def band(q, first, size):
        return held.at[q, k, pl.ds(pl.multiple_of(first, 64), size)]

    def columns(side, q):
        return feat.at[:, pl.ds(pl.multiple_of(side * kept + q * half, half), half)]

    for q in range(STEPS):
        pltpu.make_async_copy(columns(1 - h, q), sent.at[q], away_sem.at[0]).start()
        pltpu.make_async_copy(columns(h, q), band(q, cls * rows, rows), own_sem.at[0]).start()
    label_rows = kept // 128
    own_labels = labels.at[pl.ds(pl.multiple_of(h * label_rows, 8), label_rows)]
    label_copy = pltpu.make_async_copy(own_labels, labs.at[k], l_sem.at[0])
    label_copy.start()

    row8 = lax.broadcasted_iota(jnp.int32, (8, 128), 0)
    mine = jnp.full((8, 128), 40, jnp.int32)
    for s in range(5):
        mine = jnp.where(row8 == s, slots[s], mine)
    pairs[h] = mine
    coeff_row = coeffs[...].astype(F32)
    pieces = [coeff_row[:, 128 * j : 128 * (j + 1)] for j in range(4)]
    tiles[cls] = jnp.concatenate(pieces + [jnp.zeros((4, 128), F32)], axis=0)

    total[...] = jnp.zeros_like(total)
    gsum[...] = jnp.zeros_like(gsum)
    lane = lax.broadcasted_iota(jnp.int32, (8, 512), 1)
    wide_row = jnp.broadcast_to(coeff_row, (8, 512))
    diff = wide_row - 2.0 * pltpu.roll(wide_row, 511, 1) + pltpu.roll(wide_row, 510, 1)
    diff = jnp.where(lane < 510, diff, 0.0)
    pen_row[...] = diff - 2.0 * pltpu.roll(diff, 1, 1) + pltpu.roll(diff, 2, 1)

    label_copy.wait()
    pltpu.make_async_copy(sent, sent, away_sem.at[0]).wait()
    pltpu.make_async_copy(held.at[0, 0], held.at[0, 0], own_sem.at[0]).wait()
    pl.semaphore_wait(barrier, len(peers))

    def z_copy(q, c):
        return remote(sent.at[q], band(q, c * rows, rows), z_send.at[0], z_recv.at[q], antipode)

    def y_copy(q, d, c, send):
        block = band(q, c * rows, rows)
        return remote(block, block, send.at[d], y_recv.at[d, q], {"y": (up, down)[d]})

    def op_copy(q, source):
        block = band(q, source * 2 * rows, 2 * rows)
        to = {"y": jnp.where(lax.rem(q, 2) == 0, up, down)}
        return remote(block, block, op_send.at[0], op_recv.at[q], to)

    def d_copy(q, source, count):
        block = band(q, source * 2 * rows, 2 * rows * count)
        return remote(block, block, d_send.at[0], d_recv.at[q], partner)

    def tz_copy(c):
        return remote(tiles.at[c], tiles.at[c], tz_sem.at[0], tz_sem.at[1], antipode)

    def ty_copy(j, source):
        block = tiles.at[pl.ds(source * 2, 2)]
        return remote(block, block, ty_send.at[j], ty_recv.at[4 - j], {"y": lax.rem(y + j, 4)})

    def pair_copy(side):
        return remote(pairs.at[side], pairs.at[side], p_sem.at[0], p_sem.at[1], antipode)

    def label_send(core):
        return remote(labs.at[core], labs.at[core], l_sem.at[1], l_sem.at[2], partner)

    tz_copy(cls).start()
    pair_copy(h).start()
    for q in range(STEPS):
        z_copy(q, cls).start()
        for d in range(2):
            y_copy(q, d, cls, yo_send).start()
    label_send(k).start()
    tz_copy(y * 2 + 1 - h).wait_recv()
    for j in range(1, 4):
        ty_copy(j, y).start()

    def stage_a(q):
        other = y * 2 + 1 - h
        z_copy(q, other).wait_recv()
        for d in range(2):
            y_copy(q, d, other, yz_send).start()
        d_copy(q, y, 1).start()

    def stage_b(q):
        for d, source in ((0, down), (1, up)):
            block = band(q, source * 2 * rows, 2 * rows)
            remote(block, block, yo_send.at[d], y_recv.at[d, q], {"y": (up, down)[d]}).wait_recv()
        op_copy(q, jnp.where(lax.rem(q, 2) == 0, down, up)).start()
        d_copy(q, down, 1).start()
        d_copy(q, up, 1).start()

    def stage_c(q):
        op_copy(q, across).wait_recv()
        d_copy(q, across, 1).start()

    contract = (((1,), (1,)), ((), ()))

    def prepare(q):
        theirs = held.at[q, 1 - k]
        remote(theirs, theirs, d_send.at[0], d_recv.at[q], partner).wait_recv()
        weights = []
        for core in range(2):
            block = held[q, core]
            scores = jnp.dot(matrix[...].astype(BF16), block, preferred_element_type=F32)
            exponent = jnp.exp(scores - jnp.max(scores, axis=0, keepdims=True))
            probs = exponent / jnp.sum(exponent, axis=0, keepdims=True)
            weights.append(pair_weights(pairs[k], probs))
            lab_rows = [labs[core, pl.ds(q * (half // 128) + i, 1), :] for i in range(half // 128)]
            lab = jnp.concatenate(lab_rows, axis=1)
            one_hot = lax.broadcasted_iota(jnp.int32, (8, half), 0) == lab
            resid = (jnp.where(one_hot, 1.0, 0.0) - probs).astype(BF16)
            gsum[...] += lax.dot_general(resid, block, contract, preferred_element_type=F32)
        return weights

    def add_products(q, s, weights):
        term = None
        for core in range(2):
            block = held[q, core]
            scaled = (block.astype(F32) * weights[core][s : s + 1, :]).astype(BF16)
            product = lax.dot_general(scaled, block, contract, preferred_element_type=F32)
            term = product if term is None else term + product
        total[s] += term.reshape(4, 4, 32, 512)

    def step(t, carry):
        @pl.when(t < STEPS)
        def _():
            stage_a(t)

        @pl.when((t >= 1) & (t < STEPS + 1))
        def _():
            stage_b(t - 1)

        @pl.when(t >= 2)
        def _():
            stage_c(t - 2)

        @pl.when(t == 3)
        def _():
            for j in range(1, 4):
                ty_copy(4 - j, lax.rem(y + 4 - j, 4)).wait_recv()
            pair_copy(1 - h).wait_recv()
            label_send(1 - k).wait_recv()
            for c in range(CLASSES):
                tile = tiles[c]
                matrix[c : c + 1, :] = jnp.concatenate([tile[j : j + 1, :] for j in range(4)], axis=1)

        @pl.when(t >= 3)
        def _():
            weights = prepare(t - 3)
            for s in range(5):
                add_products(t - 3, s, weights)

        return carry

    lax.fori_loop(0, STEPS + 2, step, 0)

    def turn(s):
        ahead = lax.rem(k + s, 2) == 0
        return jnp.where(ahead, 1, 3), jnp.where(ahead, 3, 1)

    def around(j):
        return lax.rem(x + j, 4)

    def s_copy(s, j, source):
        tile = scales.at[source, s]
        return remote(tile, tile, s_send.at[0], s_recv.at[4 - j, s], {"x": around(j)})

    def relay_copy(s):
        return remote(relay_q.at[s], got_relay.at[s], q_send.at[0], relay_recv.at[s], {"x": around(turn(s)[0])})

    def direct_copy(s):
        return remote(direct_q.at[s], got_direct.at[s], q_send.at[1], direct_recv.at[s], {"x": around(turn(s)[1])})

    def joint_copy(s):
        return remote(joint_q.at[s], got_joint.at[s], q_send.at[2], joint_recv.at[s], {"x": around(turn(s)[0])})

    def g_copy(j, source):
        return remote(grads.at[source], grads.at[source], g_send.at[0], g_recv.at[4 - j], {"x": around(j)})

    def largest_of(block):
        top = jnp.max(jnp.max(jnp.abs(block), axis=0, keepdims=True), axis=1, keepdims=True)
        return jnp.maximum(top, 1e-30)

    def piece(s, j):
        return total[s, :, pl.ds(around(j), 1)].reshape(128, 512)

    def code(block, inverse):
        return jnp.round(block * inverse).astype(jnp.int32).astype(jnp.int16)

    def plain(block):
        return block.astype(jnp.int32).astype(F32)

    def scale_of(j, s):
        return scales[around(j), s, 0:1, 0:1]

    def first_sums(s, weights):
        add_products(STEPS - 1, s, weights)
        top = largest_of(total[s].reshape(512, 512))
        scales[x, s] = jnp.broadcast_to(top * (1.0 / LEVELS), (8, 128))
        inverse = LEVELS / top
        relay_q[s] = code(piece(s, 2), inverse)
        for j in (1, 3, 2):
            s_copy(s, j, x).start()
        relay_copy(s).start()
        direct_q[s] = code(piece(s, turn(s)[1]), inverse)
        direct_copy(s).start()

    def s_wait(s, j):
        tile = scales.at[around(j), s]
        remote(tile, tile, s_send.at[0], s_recv.at[j, s], {"x": around(j)}).wait_recv()

    def joint_sums(s):
        ahead, behind = turn(s)
        relay_copy(s).wait_recv()
        s_wait(s, behind)
        scale, own = scale_of(behind, s), scale_of(0, s)
        value = plain(got_relay[s]) * scale + piece(s, ahead)
        joint_q[s] = code(value, 1.0 / (scale + own))
        joint_copy(s).start()

    def owner(i, e):
        return {"zl": lax.rem(zl + i, 4), "zh": k, "core": lax.rem(k + e, 2)}

    def f_copy(s, i, e):
        src = coded.at[s, lax.rem(zl + i, 4), lax.rem(k + e, 2)]
        return remote(src, far.at[s, z], f_send.at[i, e], f_recv.at[s], owner(i, e))

    def fs_copy(i, e):
        src = small.at[lax.rem(zl + i, 4)]
        return remote(src, far_small.at[z], fs_send.at[i, e], fs_recv.at[0], owner(i, e))

    def to_owners(act):
        for i in (2, 1, 3, 0):
            for e in range(2):
                if i or e:
                    act(i, e)
                else:
                    pl.when(h != k)(lambda: act(0, 0))

    def last_sums(s):
        ahead, behind = turn(s)
        joint_copy(s).wait_recv()
        direct_copy(s).wait_recv()
        s_wait(s, ahead)
        s_wait(s, 2)
        value = piece(s, 0) + plain(got_joint[s]) * (scale_of(behind, s) + scale_of(2, s))
        value += plain(got_direct[s]) * scale_of(ahead, s)
        top = largest_of(value)
        out = code(value, LEVELS / top)
        for i in range(4):
            for e in range(2):
                first = i * 32 + e * 16
                coded[s, i, e] = out[first : first + 16, :]
        to_owners(lambda i, e: f_copy(s, i, e).start())
        pl.when(h == k)(lambda: pltpu.make_async_copy(coded.at[s, zl, k], far.at[s, z], f_recv.at[s]).start())
        return top * (1.0 / LEVELS)

    scale2 = jnp.zeros((8, 128), F32)
    weights = prepare(STEPS - 1)
    grads[x] = gsum[...]
    for j in (1, 3, 2):
        g_copy(j, x).start()
    for t in range(5 + 2):
        if t < 5:
            first_sums(t, weights)
        if 1 <= t < 6:
            joint_sums(t - 1)
        if t >= 2:
            scale2 = jnp.where(row8 == t - 2, last_sums(t - 2), scale2)

    for j in (1, 3, 2):
        g_copy(4 - j, around(4 - j)).wait_recv()
    all_grad = grads[0] + grads[1] + grads[2] + grads[3]
    for i in range(4):
        small[i, 0] = all_grad[:, 128 * i : 128 * (i + 1)]
        small[i, 1] = scale2
    to_owners(lambda i, e: fs_copy(i, e).start())
    pl.when(h == k)(lambda: pltpu.make_async_copy(small.at[zl], far_small.at[z], fs_recv.at[0]).start())

    row0 = zl * 128 + x * 32 + k * 16
    ia = lax.broadcasted_iota(jnp.int32, (16, 512), 0) + row0
    ib = lax.broadcasted_iota(jnp.int32, (16, 512), 1)
    pen = jnp.zeros((16, 512), F32)
    taps = (1.0, -2.0, 1.0)
    for m in range(3):
        inside = (ia - m >= 0) & (ia - m <= 509)
        for n in range(3):
            pen += jnp.where(inside & (ib - n == ia - m), taps[m] * taps[n], 0.0)

    pltpu.make_async_copy(far_small, far_small, fs_recv.at[0]).wait()
    summed = far_small[0, 0]
    for source in range(1, 8):
        summed += far_small[source, 0]
    picked = jnp.sum(jnp.where(row8 == cls, summed, 0.0), axis=0, keepdims=True) * (1.0 / 4096.0)
    pen_part = pen_row[:, pl.ds(pl.multiple_of(zl * 128, 128), 128)]
    final = picked - smoothing[cls] * pen_part
    stage[...] = pltpu.roll(final, lax.rem(128 - (x * 32 + k * 16), 128), 1)
    grad_out[...] = stage[0:1, 0:16]
    for s in range(5):
        pltpu.make_async_copy(far.at[s], far.at[s], f_recv.at[s]).wait()
        value = jnp.zeros((16, 512), F32)
        for source in range(8):
            value += plain(far[s, source]) * far_small[source, 1, s : s + 1, 0:1]
        smooth = jnp.float32(0.0)
        for j, number in enumerate(DIAGONAL):
            smooth += jnp.where(slots[s] == number, smoothing[j], 0.0)
        hess_out[s] = value * (1.0 / 4096.0) + pen * smooth

    def sent_all(ref, sem):
        pltpu.make_async_copy(ref, ref, sem).wait()

    tz_copy(cls).wait_send()
    pair_copy(h).wait_send()
    label_send(k).wait_send()
    for j in range(1, 4):
        ty_copy(j, y).wait_send()
    sent_all(sent, z_send.at[0])
    for d in range(2):
        sent_all(held.at[0, 0], yo_send.at[d])
        sent_all(held.at[0, 0], yz_send.at[d])
    sent_all(held.at[0], op_send.at[0])
    sent_all(held.at[pl.ds(0, STEPS // 2)], d_send.at[0])
    sent_all(scales.at[pl.ds(0, 3)], s_send.at[0])
    for i in range(3):
        sent_all(relay_q, q_send.at[i])
    sent_all(grads.at[pl.ds(0, 3)], g_send.at[0])
    to_owners(lambda i, e: sent_all(coded.at[:, 0, 0], f_send.at[i, e]))
    to_owners(lambda i, e: fs_copy(i, e).wait_send())


def local(features, labels, coeffs, smoothing, pair_slots):
    vmem = pl.BlockSpec(memory_space=pltpu.VMEM)
    smem = pl.BlockSpec(memory_space=pltpu.SMEM)
    anyspace = pl.BlockSpec(memory_space=pl.ANY)
    dma = pltpu.SemaphoreType.DMA
    half = features.shape[1] // 2 // STEPS
    block = pltpu.VMEM((5, 128, 512), jnp.int16)
    hessian, gradient = pl.pallas_call(
        newton_kernel,
        out_shape=(
            jax.ShapeDtypeStruct((5, 16, 512), F32),
            jax.ShapeDtypeStruct((1, 16), F32),
        ),
        in_specs=[anyspace, vmem, anyspace, smem, smem],
        out_specs=(vmem, vmem),
        scratch_shapes=[
            pltpu.VMEM((STEPS, 2, 512, half), BF16),
            pltpu.VMEM((STEPS, 64, half), BF16),
            pltpu.VMEM((5, 4, 4, 32, 512), F32),
            pltpu.VMEM((2, 16, 128), jnp.int32),
            pltpu.VMEM((2, 8, 128), jnp.int32),
            pltpu.VMEM((8, 8, 128), F32),
            pltpu.VMEM((8, 512), F32),
            pltpu.VMEM((8, 512), F32),
            pltpu.VMEM((4, 5, 8, 128), F32),
            block, block, block, block, block, block,
            pltpu.VMEM((4, 8, 512), F32),
            pltpu.VMEM((5, 4, 2, 16, 512), jnp.int16),
            pltpu.VMEM((4, 2, 8, 128), F32),
            pltpu.VMEM((5, 8, 16, 512), jnp.int16),
            pltpu.VMEM((8, 2, 8, 128), F32),
            pltpu.VMEM((8, 512), F32),
            pltpu.VMEM((8, 128), F32),
            dma((1,)), dma((1,)), dma((1,)), dma((STEPS,)), dma((2,)), dma((2,)), dma((2, STEPS)),
            dma((1,)), dma((STEPS,)), dma((1,)), dma((STEPS,)),
            dma((2,)), dma((4,)), dma((4,)), dma((2,)), dma((3,)),
            dma((1,)), dma((4, 5)), dma((3,)), dma((5,)), dma((5,)), dma((5,)),
            dma((1,)), dma((4,)), dma((4, 2)), dma((5,)), dma((4, 2)), dma((1,)),
        ],
        compiler_params=pltpu.CompilerParams(collective_id=0, has_side_effects=True),
        name="newton",
    )(features, coeffs, labels.reshape(32, 128), pair_slots, smoothing)
    return hessian.transpose(1, 0, 2), gradient


def solution(mesh):
    finer = Mesh(mesh.devices.reshape(4, 4, 2, 4, 2), AXES)
    placed = (P(CLS, DP), P(DP), P(CLS, None), P(), P(CLS))
    return jax.shard_map(
        local,
        mesh=finer,
        in_specs=placed,
        out_specs=(P(DP, CLS, None), P(CLS, DP)),
        check_vma=False,
    )
```

```python
import jax
import jax.numpy as jnp
from jax import lax
from jax.experimental import pallas as pl
from jax.experimental.pallas import tpu as pltpu
from jax.sharding import Mesh
from jax.sharding import PartitionSpec as P

CLASSES = 8
PAIRS = CLASSES * (CLASSES + 1) // 2
STARTS = (8, 15, 21, 26, 30, 33, 35)
DIAGONAL = (0, 8, 15, 21, 26, 30, 33, 35)
AXES = ("zl", "x", "core", "y", "zh")
DP = ("zl", "x", "core")
CLS = ("y", "zh")
MESH = pl.DeviceIdType.MESH
STEPS = 8
LEVELS = 32767.0
ORDER = (
    ("beta", 4), ("first", 0), ("first", 1), ("joint", 0), ("first", 2), ("joint", 1), ("last", 0), ("first", 3),
    ("joint", 2), ("last", 1), ("joint", 3), ("last", 2), ("cross", 4), ("last", 3),
)
F32 = jnp.float32
BF16 = jnp.bfloat16


def place():
    return {name: lax.axis_index(name) for name in AXES}


def remote(src, dst, send, recv, device):
    return pltpu.make_async_remote_copy(
        src_ref=src, dst_ref=dst, send_sem=send, recv_sem=recv, device_id=device, device_id_type=MESH
    )


def pair_weights(slots, probs):
    pair = jnp.minimum(slots, PAIRS - 1)
    first = jnp.zeros_like(pair)
    start = jnp.zeros_like(pair)
    for before, at in zip((0,) + STARTS, STARTS):
        later = pair >= at
        first += jnp.where(later, 1, 0)
        start += jnp.where(later, at - before, 0)
    second = pair - start + first
    live = (slots < PAIRS)[:, :1]
    first, second = first[:, :1], second[:, :1]
    prob_first = jnp.zeros_like(probs)
    prob_second = jnp.zeros_like(probs)
    for k in range(CLASSES):
        row = probs[k : k + 1, :]
        prob_first += jnp.where(first == k, row, 0.0)
        prob_second += jnp.where(second == k, row, 0.0)
    same = jnp.where(first == second, 1.0, 0.0)
    return jnp.where(live, prob_first * (same - prob_second), 0.0)


def newton_kernel(
    feat, coeffs, labels, slots, smoothing,
    hess_out, grad_out,
    held, sent, total, labs, pairs, tiles, matrix, factors, resids, gsum, scales,
    relay_q, direct_q, joint_q, got_relay, got_direct, got_joint, grads,
    coded, small, far, far_small, b_q, b_scale, far_b, far_bs, b_sum, got_b, pen_row, stage,
    own_sem, away_sem, z_send, z_recv, yo_send, yz_send, y_recv, op_send, op_recv, d_send, d_recv,
    tz_sem, ty_send, ty_recv, p_sem, l_sem, s_send, s_recv, q_send, relay_recv, direct_recv, joint_recv,
    g_send, g_recv, f_send, f_recv, fs_send, fs_recv, b_send, b_recv, bs_send, bs_recv, bx_send, bx_recv,
):
    at = place()
    k, x, y, h, zl = at["core"], at["x"], at["y"], at["zh"], at["zl"]
    z = h * 4 + zl
    cls = y * 2 + h
    half = held.shape[3]
    rows = feat.shape[0]
    kept = feat.shape[1] // 2
    up, down, across = lax.rem(y + 1, 4), lax.rem(y + 3, 4), lax.rem(y + 2, 4)
    antipode, partner = {"zh": 1 - h}, {"core": 1 - k}

    peers = [{"x": lax.rem(x + j, 4)} for j in range(1, 4)] + [{"y": lax.rem(y + j, 4)} for j in range(1, 4)]
    for a in range(2):
        for i in range(4):
            for e in range(2):
                if a or i or e:
                    peers.append({"zl": lax.rem(zl + i, 4), "zh": lax.rem(h + a, 2), "core": lax.rem(k + e, 2)})
    barrier = pltpu.get_barrier_semaphore()
    for device in peers[::-1]:
        pl.semaphore_signal(barrier, inc=1, device_id=device, device_id_type=MESH)

    def band(q, first, size):
        return held.at[q, k, pl.ds(pl.multiple_of(first, 64), size)]

    def columns(side, q):
        return feat.at[:, pl.ds(pl.multiple_of(side * kept + q * half, half), half)]

    for q in range(STEPS):
        pltpu.make_async_copy(columns(1 - h, q), sent.at[q], away_sem.at[0]).start()
        pltpu.make_async_copy(columns(h, q), band(q, cls * rows, rows), own_sem.at[0]).start()
    label_rows = kept // 128
    own_labels = labels.at[pl.ds(pl.multiple_of(h * label_rows, 8), label_rows)]
    label_copy = pltpu.make_async_copy(own_labels, labs.at[k], l_sem.at[0])
    label_copy.start()

    row8 = lax.broadcasted_iota(jnp.int32, (8, 128), 0)
    mine = jnp.full((8, 128), 40, jnp.int32)
    for s in range(5):
        mine = jnp.where(row8 == s, slots[s], mine)
    pairs[h] = mine
    coeff_row = coeffs[...].astype(F32)
    pieces = [coeff_row[:, 128 * j : 128 * (j + 1)] for j in range(4)]
    tiles[cls] = jnp.concatenate(pieces + [jnp.zeros((4, 128), F32)], axis=0)

    total[...] = jnp.zeros_like(total)
    gsum[...] = jnp.zeros_like(gsum)
    lane = lax.broadcasted_iota(jnp.int32, (8, 512), 1)
    wide_row = jnp.broadcast_to(coeff_row, (8, 512))
    diff = wide_row - 2.0 * pltpu.roll(wide_row, 511, 1) + pltpu.roll(wide_row, 510, 1)
    diff = jnp.where(lane < 510, diff, 0.0)
    pen_row[...] = diff - 2.0 * pltpu.roll(diff, 1, 1) + pltpu.roll(diff, 2, 1)

    label_copy.wait()
    pltpu.make_async_copy(sent, sent, away_sem.at[0]).wait()
    pltpu.make_async_copy(held.at[0, 0], held.at[0, 0], own_sem.at[0]).wait()
    pl.semaphore_wait(barrier, len(peers))

    def z_copy(q, c):
        return remote(sent.at[q], band(q, c * rows, rows), z_send.at[0], z_recv.at[q], antipode)

    def y_copy(q, d, c, send):
        block = band(q, c * rows, rows)
        return remote(block, block, send.at[d], y_recv.at[d, q], {"y": (up, down)[d]})

    def op_copy(q, source):
        block = band(q, source * 2 * rows, 2 * rows)
        to = {"y": jnp.where(lax.rem(q, 2) == 0, up, down)}
        return remote(block, block, op_send.at[0], op_recv.at[q], to)

    def d_copy(q, source, count):
        block = band(q, source * 2 * rows, 2 * rows * count)
        return remote(block, block, d_send.at[0], d_recv.at[q], partner)

    def tz_copy(c):
        return remote(tiles.at[c], tiles.at[c], tz_sem.at[0], tz_sem.at[1], antipode)

    def ty_copy(j, source):
        block = tiles.at[pl.ds(source * 2, 2)]
        return remote(block, block, ty_send.at[j], ty_recv.at[4 - j], {"y": lax.rem(y + j, 4)})

    def pair_copy(side):
        return remote(pairs.at[side], pairs.at[side], p_sem.at[0], p_sem.at[1], antipode)

    def label_send(core):
        return remote(labs.at[core], labs.at[core], l_sem.at[1], l_sem.at[2], partner)

    tz_copy(cls).start()
    pair_copy(h).start()
    for q in range(STEPS):
        z_copy(q, cls).start()
        for d in range(2):
            y_copy(q, d, cls, yo_send).start()
    label_send(k).start()
    tz_copy(y * 2 + 1 - h).wait_recv()
    for j in range(1, 4):
        ty_copy(j, y).start()

    def stage_a(q):
        other = y * 2 + 1 - h
        z_copy(q, other).wait_recv()
        for d in range(2):
            y_copy(q, d, other, yz_send).start()
        d_copy(q, y, 1).start()

    def stage_b(q):
        for d, source in ((0, down), (1, up)):
            block = band(q, source * 2 * rows, 2 * rows)
            remote(block, block, yo_send.at[d], y_recv.at[d, q], {"y": (up, down)[d]}).wait_recv()
        op_copy(q, jnp.where(lax.rem(q, 2) == 0, down, up)).start()
        d_copy(q, down, 1).start()
        d_copy(q, up, 1).start()

    def stage_c(q):
        op_copy(q, across).wait_recv()
        d_copy(q, across, 1).start()

    contract = (((1,), (1,)), ((), ()))

    def wait_partner(q):
        theirs = held.at[q, 1 - k]
        remote(theirs, theirs, d_send.at[0], d_recv.at[q], partner).wait_recv()

    def prepare(q):
        both = [jnp.dot(matrix[...].astype(BF16), held[q, core], preferred_element_type=F32) for core in range(2)]
        scores = jnp.concatenate(both, axis=1)
        exponent = jnp.exp(scores - jnp.max(scores, axis=0, keepdims=True))
        probs = exponent / jnp.sum(exponent, axis=0, keepdims=True)
        turn = lax.rem(q, 2)
        factors[turn] = pair_weights(pairs[k], probs)
        lab_rows = [
            labs[core, pl.ds(q * (half // 128) + i, 1), :] for core in range(2) for i in range(half // 128)
        ]
        lab = jnp.concatenate(lab_rows, axis=1)
        one_hot = lax.broadcasted_iota(jnp.int32, (8, 2 * half), 0) == lab
        resids[turn] = jnp.where(one_hot, 1.0, 0.0) - probs

    def add_products(q, s):
        turn = lax.rem(q, 2)
        left, right, extra = None, None, None
        for core in range(2):
            block = held[q, core]
            span = slice(core * half, (core + 1) * half)
            scaled = (block.astype(F32) * factors[turn, s : s + 1, span]).astype(BF16)
            first = lax.dot_general(scaled[:256], block[:256], contract, preferred_element_type=F32)
            second = lax.dot_general(scaled, block[256:], contract, preferred_element_type=F32)
            left = first if left is None else left + first
            right = second if right is None else right + second
            if s == 0:
                resid = resids[turn, :, span].astype(BF16)
                term = lax.dot_general(resid, block, contract, preferred_element_type=F32)
                extra = term if extra is None else extra + term
        total[s, 0:2, :, :, 0:256] += left.reshape(2, 4, 32, 256)
        total[s, :, :, :, 256:512] += right.reshape(4, 4, 32, 256)
        if s == 0:
            gsum[...] += extra

    for t in range(6):
        stage_a(t)
        if t >= 2:
            stage_b(t - 2)
        if t >= 4:
            stage_c(t - 4)
    for j in range(1, 4):
        ty_copy(4 - j, lax.rem(y + 4 - j, 4)).wait_recv()
    pair_copy(1 - h).wait_recv()
    label_send(1 - k).wait_recv()
    for c in range(CLASSES):
        tile = tiles[c]
        matrix[c : c + 1, :] = jnp.concatenate([tile[j : j + 1, :] for j in range(4)], axis=1)
    wait_partner(0)
    prepare(0)

    def step(t, carry):
        for stage, first in ((stage_a, 6), (stage_b, 4), (stage_c, 2)):

            @pl.when(t < STEPS - first)
            def _():
                stage(t + first)

        wait_partner(t + 1)
        for s in range(5):
            add_products(t, s)
            if s == 0:
                prepare(t + 1)
        return carry

    lax.fori_loop(0, STEPS - 1, step, 0)

    def turn(s):
        ahead = lax.rem(k + s, 2) == 0
        return jnp.where(ahead, 1, 3), jnp.where(ahead, 3, 1)

    def around(j):
        return lax.rem(x + j, 4)

    def s_copy(s, j, source):
        tile = scales.at[source, s]
        return remote(tile, tile, s_send.at[0], s_recv.at[4 - j, s], {"x": around(j)})

    def relay_copy(s):
        return remote(relay_q.at[s], got_relay.at[s], q_send.at[0], relay_recv.at[s], {"x": around(turn(s)[0])})

    def direct_copy(s):
        return remote(direct_q.at[s], got_direct.at[s], q_send.at[1], direct_recv.at[s], {"x": around(turn(s)[1])})

    def joint_copy(s):
        return remote(joint_q.at[s], got_joint.at[s], q_send.at[2], joint_recv.at[s], {"x": around(turn(s)[0])})

    def g_copy(j, source):
        return remote(grads.at[source], grads.at[source], g_send.at[0], g_recv.at[4 - j], {"x": around(j)})

    def largest_of(block):
        top = jnp.max(jnp.max(jnp.abs(block), axis=0, keepdims=True), axis=1, keepdims=True)
        return jnp.maximum(top, 1e-30)

    def piece(s, j):
        return total[s, :, pl.ds(around(j), 1)].reshape(128, 512)

    def code(block, inverse):
        return jnp.round(block * inverse).astype(jnp.int32).astype(jnp.int16)

    def plain(block):
        return block.astype(jnp.int32).astype(F32)

    def scale_of(j, s):
        return scales[around(j), s, 0:1, 0:1]

    def finish(s):
        add_products(STEPS - 1, s)
        corner = total[s, 0:2, :, :, 256:512].reshape(256, 256)
        total[s, 2:4, :, :, 0:256] = corner.T.reshape(2, 4, 32, 256)

    def first_sums(s):
        finish(s)
        top = largest_of(total[s].reshape(512, 512))
        scales[x, s] = jnp.broadcast_to(top * (1.0 / LEVELS), (8, 128))
        inverse = LEVELS / top
        relay_q[s] = code(piece(s, 2), inverse)
        for j in (1, 3, 2):
            s_copy(s, j, x).start()
        relay_copy(s).start()
        direct_q[s] = code(piece(s, turn(s)[1]), inverse)
        direct_copy(s).start()

    def s_wait(s, j):
        tile = scales.at[around(j), s]
        remote(tile, tile, s_send.at[0], s_recv.at[j, s], {"x": around(j)}).wait_recv()

    def joint_sums(s):
        ahead, behind = turn(s)
        relay_copy(s).wait_recv()
        s_wait(s, behind)
        scale, own = scale_of(behind, s), scale_of(0, s)
        value = plain(got_relay[s]) * scale + piece(s, ahead)
        joint_q[s] = code(value, 1.0 / (scale + own))
        joint_copy(s).start()

    def owner(i, e):
        return {"zl": lax.rem(zl + i, 4), "zh": k, "core": lax.rem(k + e, 2)}

    def f_copy(s, i, e):
        src = coded.at[s, lax.rem(zl + i, 4), lax.rem(k + e, 2)]
        return remote(src, far.at[s, z], f_send.at[i, e], f_recv.at[s], owner(i, e))

    def fs_copy(i, e):
        src = small.at[lax.rem(zl + i, 4)]
        return remote(src, far_small.at[z], fs_send.at[i, e], fs_recv.at[0], owner(i, e))

    def to_owners(act):
        for i in (2, 1, 3, 0):
            for e in range(2):
                if i or e:
                    act(i, e)
                else:
                    pl.when(h != k)(lambda: act(0, 0))

    def last_sums(s):
        ahead, behind = turn(s)
        joint_copy(s).wait_recv()
        direct_copy(s).wait_recv()
        s_wait(s, ahead)
        s_wait(s, 2)
        value = piece(s, 0) + plain(got_direct[s]) * scale_of(ahead, s)
        value += plain(got_joint[s]) * (scale_of(behind, s) + scale_of(2, s))
        top = largest_of(value)
        out = code(value, LEVELS / top)
        for i in range(4):
            for e in range(2):
                first = i * 32 + e * 16
                coded[s, i, e] = out[first : first + 16, :]
        to_owners(lambda i, e: f_copy(s, i, e).start())
        pl.when(h == k)(lambda: pltpu.make_async_copy(coded.at[s, zl, k], far.at[s, z], f_recv.at[s]).start())
        return top * (1.0 / LEVELS)

    def b_copy(i, e):
        src = b_q.at[lax.rem(zl + i, 4), lax.rem(k + e, 2)]
        return remote(src, far_b.at[z], b_send.at[i, e], b_recv.at[0], owner(i, e))

    def bs_copy(i, e):
        return remote(b_scale, far_bs.at[z], bs_send.at[i, e], bs_recv.at[0], owner(i, e))

    def bx_copy(j, source):
        return remote(b_sum.at[around(j)], got_b.at[source], bx_send.at[0], bx_recv.at[4 - j], {"x": around(j)})

    def beta_sums(s):
        finish(s)
        top = largest_of(total[s].reshape(512, 512))
        b_scale[...] = jnp.broadcast_to(top * (1.0 / LEVELS), (8, 128))
        inverse = LEVELS / top
        for i in range(4):
            for c in range(2):
                for p in range(4):
                    b_q[i, c, 16 * p : 16 * (p + 1), :] = code(total[s, i, p, 16 * c : 16 * (c + 1), :], inverse)
        to_owners(lambda i, e: b_copy(i, e).start())
        to_owners(lambda i, e: bs_copy(i, e).start())

        @pl.when(h == k)
        def _():
            pltpu.make_async_copy(b_q.at[zl, k], far_b.at[z], b_recv.at[0]).start()
            pltpu.make_async_copy(b_scale, far_bs.at[z], bs_recv.at[0]).start()

    def cross_sums():
        pltpu.make_async_copy(far_b, far_b, b_recv.at[0]).wait()
        pltpu.make_async_copy(far_bs, far_bs, bs_recv.at[0]).wait()
        value = jnp.zeros((64, 512), F32)
        for source in range(8):
            value += plain(far_b[source]) * far_bs[source, 0:1, 0:1]
        b_sum[...] = value.reshape(4, 16, 512)
        for j in (1, 3, 2):
            bx_copy(j, x).start()

    scale2 = jnp.zeros((8, 128), F32)
    for act, s in ORDER:
        if act == "beta":
            beta_sums(s)
        if act == "cross":
            cross_sums()
        if act == "first":
            first_sums(s)
            if s == 0:
                grads[x] = gsum[...]
                for j in (1, 3, 2):
                    g_copy(j, x).start()
        if act == "joint":
            joint_sums(s)
        if act == "last":
            scale2 = jnp.where(row8 == s, last_sums(s), scale2)

    for j in (1, 3, 2):
        g_copy(4 - j, around(4 - j)).wait_recv()
    all_grad = grads[0] + grads[1] + grads[2] + grads[3]
    for i in range(4):
        small[i, 0] = all_grad[:, 128 * i : 128 * (i + 1)]
        small[i, 1] = scale2
    to_owners(lambda i, e: fs_copy(i, e).start())
    pl.when(h == k)(lambda: pltpu.make_async_copy(small.at[zl], far_small.at[z], fs_recv.at[0]).start())

    row0 = zl * 128 + x * 32 + k * 16
    ia = lax.broadcasted_iota(jnp.int32, (16, 512), 0) + row0
    ib = lax.broadcasted_iota(jnp.int32, (16, 512), 1)
    pen = jnp.zeros((16, 512), F32)
    taps = (1.0, -2.0, 1.0)
    for m in range(3):
        inside = (ia - m >= 0) & (ia - m <= 509)
        for n in range(3):
            pen += jnp.where(inside & (ib - n == ia - m), taps[m] * taps[n], 0.0)

    pltpu.make_async_copy(far_small, far_small, fs_recv.at[0]).wait()
    summed = far_small[0, 0]
    for source in range(1, 8):
        summed += far_small[source, 0]
    picked = jnp.sum(jnp.where(row8 == cls, summed, 0.0), axis=0, keepdims=True) * (1.0 / 4096.0)
    pen_part = pen_row[:, pl.ds(pl.multiple_of(zl * 128, 128), 128)]
    final = picked - smoothing[cls] * pen_part
    stage[...] = pltpu.roll(final, lax.rem(128 - (x * 32 + k * 16), 128), 1)
    grad_out[...] = stage[0:1, 0:16]
    for s in range(5):
        if s == 4:
            value = b_sum[x]
            for j in (1, 3, 2):
                bx_copy(4 - j, around(j)).wait_recv()
                value += got_b[around(j)]
        else:
            pltpu.make_async_copy(far.at[s], far.at[s], f_recv.at[s]).wait()
            value = jnp.zeros((16, 512), F32)
            for source in range(8):
                value += plain(far[s, source]) * far_small[source, 1, s : s + 1, 0:1]
        smooth = jnp.float32(0.0)
        for j, number in enumerate(DIAGONAL):
            smooth += jnp.where(slots[s] == number, smoothing[j], 0.0)
        hess_out[s] = value * (1.0 / 4096.0) + pen * smooth

    def sent_all(ref, sem):
        pltpu.make_async_copy(ref, ref, sem).wait()

    tz_copy(cls).wait_send()
    pair_copy(h).wait_send()
    label_send(k).wait_send()
    for j in range(1, 4):
        ty_copy(j, y).wait_send()
    sent_all(sent, z_send.at[0])
    for d in range(2):
        sent_all(held.at[0, 0], yo_send.at[d])
        sent_all(held.at[0, 0], yz_send.at[d])
    sent_all(held.at[0], op_send.at[0])
    sent_all(held.at[pl.ds(0, STEPS // 2)], d_send.at[0])
    sent_all(scales.at[pl.ds(0, 3)], s_send.at[0])
    sent_all(got_b.at[pl.ds(0, 3)], bx_send.at[0])
    to_owners(lambda i, e: b_copy(i, e).wait_send())
    to_owners(lambda i, e: bs_copy(i, e).wait_send())
    for i in range(3):
        sent_all(relay_q, q_send.at[i])
    sent_all(grads.at[pl.ds(0, 3)], g_send.at[0])
    to_owners(lambda i, e: sent_all(coded.at[:, 0, 0], f_send.at[i, e]))
    to_owners(lambda i, e: fs_copy(i, e).wait_send())


def local(features, labels, coeffs, smoothing, pair_slots):
    vmem = pl.BlockSpec(memory_space=pltpu.VMEM)
    smem = pl.BlockSpec(memory_space=pltpu.SMEM)
    anyspace = pl.BlockSpec(memory_space=pl.ANY)
    dma = pltpu.SemaphoreType.DMA
    half = features.shape[1] // 2 // STEPS
    block = pltpu.VMEM((4, 128, 512), jnp.int16)
    hessian, gradient = pl.pallas_call(
        newton_kernel,
        out_shape=(
            jax.ShapeDtypeStruct((5, 16, 512), F32),
            jax.ShapeDtypeStruct((1, 16), F32),
        ),
        in_specs=[anyspace, vmem, anyspace, smem, smem],
        out_specs=(vmem, vmem),
        scratch_shapes=[
            pltpu.VMEM((STEPS, 2, 512, half), BF16),
            pltpu.VMEM((STEPS, 64, half), BF16),
            pltpu.VMEM((5, 4, 4, 32, 512), F32),
            pltpu.VMEM((2, 16, 128), jnp.int32),
            pltpu.VMEM((2, 8, 128), jnp.int32),
            pltpu.VMEM((8, 8, 128), F32),
            pltpu.VMEM((8, 512), F32),
            pltpu.VMEM((2, 8, 2 * half), F32),
            pltpu.VMEM((2, 8, 2 * half), F32),
            pltpu.VMEM((8, 512), F32),
            pltpu.VMEM((4, 4, 8, 128), F32),
            block, block, block, block, block, block,
            pltpu.VMEM((4, 8, 512), F32),
            pltpu.VMEM((4, 4, 2, 16, 512), jnp.int16),
            pltpu.VMEM((4, 2, 8, 128), F32),
            pltpu.VMEM((4, 8, 16, 512), jnp.int16),
            pltpu.VMEM((8, 2, 8, 128), F32),
            pltpu.VMEM((4, 2, 64, 512), jnp.int16),
            pltpu.VMEM((8, 128), F32),
            pltpu.VMEM((8, 64, 512), jnp.int16),
            pltpu.VMEM((8, 8, 128), F32),
            pltpu.VMEM((4, 16, 512), F32),
            pltpu.VMEM((4, 16, 512), F32),
            pltpu.VMEM((8, 512), F32),
            pltpu.VMEM((8, 128), F32),
            dma((1,)), dma((1,)), dma((1,)), dma((STEPS,)), dma((2,)), dma((2,)), dma((2, STEPS)),
            dma((1,)), dma((STEPS,)), dma((1,)), dma((STEPS,)),
            dma((2,)), dma((4,)), dma((4,)), dma((2,)), dma((3,)),
            dma((1,)), dma((4, 4)), dma((3,)), dma((4,)), dma((4,)), dma((4,)),
            dma((1,)), dma((4,)), dma((4, 2)), dma((4,)), dma((4, 2)), dma((1,)),
            dma((4, 2)), dma((1,)), dma((4, 2)), dma((1,)), dma((1,)), dma((4,)),
        ],
        compiler_params=pltpu.CompilerParams(collective_id=0, has_side_effects=True),
        name="newton",
    )(features, coeffs, labels.reshape(32, 128), pair_slots, smoothing)
    return hessian.transpose(1, 0, 2), gradient


def solution(mesh):
    finer = Mesh(mesh.devices.reshape(4, 4, 2, 4, 2), AXES)
    placed = (P(CLS, DP), P(DP), P(CLS, None), P(), P(CLS))
    return jax.shard_map(
        local,
        mesh=finer,
        in_specs=placed,
        out_specs=(P(DP, CLS, None), P(CLS, DP)),
        check_vma=False,
    )
```

```python
import jax
import jax.numpy as jnp
from jax import lax
from jax.experimental import pallas as pl
from jax.experimental.pallas import tpu as pltpu
from jax.sharding import Mesh
from jax.sharding import PartitionSpec as P

CLASSES = 8
PAIRS = CLASSES * (CLASSES + 1) // 2
STARTS = (8, 15, 21, 26, 30, 33, 35)
DIAGONAL = (0, 8, 15, 21, 26, 30, 33, 35)
AXES = ("zl", "x", "core", "y", "zh")
DP = ("zl", "x", "core")
CLS = ("y", "zh")
MESH = pl.DeviceIdType.MESH
STEPS = 8
AROUND = 4
LEVELS = 32767.0
ORDER = (
    ("first", 0, 0), ("first", 1, 0), ("beta", 4, 0), ("joint", 0, 0), ("joint", 0, 1), ("first", 2, 0), ("joint", 1, 0), ("joint", 1, 1), ("first", 3, 0),
    ("last", 0, 0), ("joint", 2, 0), ("last", 0, 1), ("joint", 2, 1), ("last", 1, 0), ("joint", 3, 0), ("last", 1, 1), ("joint", 3, 1),
    ("last", 2, 0), ("last", 2, 1), ("cross", 4, 0), ("last", 3, 0), ("last", 3, 1),
)
F32 = jnp.float32
BF16 = jnp.bfloat16


def place():
    return {name: lax.axis_index(name) for name in AXES}


def remote(src, dst, send, recv, device):
    return pltpu.make_async_remote_copy(
        src_ref=src, dst_ref=dst, send_sem=send, recv_sem=recv, device_id=device, device_id_type=MESH
    )


def pair_weights(slots, probs):
    pair = jnp.minimum(slots, PAIRS - 1)
    first = jnp.zeros_like(pair)
    start = jnp.zeros_like(pair)
    for before, at in zip((0,) + STARTS, STARTS):
        later = pair >= at
        first += jnp.where(later, 1, 0)
        start += jnp.where(later, at - before, 0)
    second = pair - start + first
    live = (slots < PAIRS)[:, :1]
    first, second = first[:, :1], second[:, :1]
    prob_first = jnp.zeros_like(probs)
    prob_second = jnp.zeros_like(probs)
    for k in range(CLASSES):
        row = probs[k : k + 1, :]
        prob_first += jnp.where(first == k, row, 0.0)
        prob_second += jnp.where(second == k, row, 0.0)
    same = jnp.where(first == second, 1.0, 0.0)
    return jnp.where(live, prob_first * (same - prob_second), 0.0)


def newton_kernel(
    feat, coeffs, labels, slots, smoothing,
    hess_out, grad_out,
    held, sent, total, labs, pairs, tiles, matrix, factors, resids, later_factors, later_resids, gsum, scales,
    relay_q, direct_q, joint_q, got_relay, got_direct, got_joint, grads,
    coded, small, far, far_small, b_q, b_scale, far_b, far_bs, b_sum, got_b, pen_row, stage,
    own_sem, away_sem, z_send, z_recv, yo_send, yz_send, y_recv, op_send, op_recv, d_send, d_recv,
    tz_sem, ty_send, ty_recv, p_sem, l_sem, s_send, s_recv, q_send, relay_recv, direct_recv, joint_recv,
    g_send, g_recv, f_send, f_recv, fs_send, fs_recv, b_send, b_recv, bs_send, bs_recv, bx_send, bx_recv,
):
    at = place()
    k, x, y, h, zl = at["core"], at["x"], at["y"], at["zh"], at["zl"]
    z = h * 4 + zl
    cls = y * 2 + h
    half = held.shape[3]
    rows = feat.shape[0]
    kept = feat.shape[1] // 2
    up, down, across = lax.rem(y + 1, 4), lax.rem(y + 3, 4), lax.rem(y + 2, 4)
    antipode, partner = {"zh": 1 - h}, {"core": 1 - k}

    peers = [{"x": lax.rem(x + j, 4)} for j in range(1, 4)] + [{"y": lax.rem(y + j, 4)} for j in range(1, 4)]
    for a in range(2):
        for i in range(4):
            for e in range(2):
                if a or i or e:
                    peers.append({"zl": lax.rem(zl + i, 4), "zh": lax.rem(h + a, 2), "core": lax.rem(k + e, 2)})
    barrier = pltpu.get_barrier_semaphore()
    for device in peers[::-1]:
        pl.semaphore_signal(barrier, inc=1, device_id=device, device_id_type=MESH)

    def band(q, first, size):
        return held.at[q, k, pl.ds(pl.multiple_of(first, 64), size)]

    def columns(side, q):
        return feat.at[:, pl.ds(pl.multiple_of(side * kept + q * half, half), half)]

    for q in range(STEPS):
        pltpu.make_async_copy(columns(1 - h, q), sent.at[q], away_sem.at[0]).start()
        pltpu.make_async_copy(columns(h, q), band(q, cls * rows, rows), own_sem.at[0]).start()
    label_rows = kept // 128
    own_labels = labels.at[pl.ds(pl.multiple_of(h * label_rows, 8), label_rows)]
    label_copy = pltpu.make_async_copy(own_labels, labs.at[k], l_sem.at[0])
    label_copy.start()

    row8 = lax.broadcasted_iota(jnp.int32, (8, 128), 0)
    mine = jnp.full((8, 128), 40, jnp.int32)
    for s in range(5):
        mine = jnp.where(row8 == s, slots[s], mine)
    pairs[h] = mine
    coeff_row = coeffs[...].astype(F32)
    pieces = [coeff_row[:, 128 * j : 128 * (j + 1)] for j in range(4)]
    tiles[cls] = jnp.concatenate(pieces + [jnp.zeros((4, 128), F32)], axis=0)

    pl.semaphore_wait(barrier, len(peers))
    pltpu.make_async_copy(sent, sent, away_sem.at[0]).wait()
    pltpu.make_async_copy(held.at[0, 0], held.at[0, 0], own_sem.at[0]).wait()
    label_copy.wait()

    def z_copy(q, c):
        return remote(sent.at[q], band(q, c * rows, rows), z_send.at[0], z_recv.at[q], antipode)

    def y_copy(q, d, c, send):
        block = band(q, c * rows, rows)
        return remote(block, block, send.at[d], y_recv.at[d, q], {"y": (up, down)[d]})

    def op_copy(q, source):
        block = band(q, source * 2 * rows, 2 * rows)
        to = {"y": jnp.where(lax.rem(q, 2) == 0, up, down)}
        return remote(block, block, op_send.at[0], op_recv.at[q], to)

    def d_copy(q, source, count):
        block = band(q, source * 2 * rows, 2 * rows * count)
        return remote(block, block, d_send.at[0], d_recv.at[q], partner)

    def tz_copy(c):
        return remote(tiles.at[c], tiles.at[c], tz_sem.at[0], tz_sem.at[1], antipode)

    def ty_copy(j, source):
        block = tiles.at[pl.ds(source * 2, 2)]
        return remote(block, block, ty_send.at[j], ty_recv.at[4 - j], {"y": lax.rem(y + j, 4)})

    def pair_copy(side):
        return remote(pairs.at[side], pairs.at[side], p_sem.at[0], p_sem.at[1], antipode)

    def label_send(core):
        return remote(labs.at[core], labs.at[core], l_sem.at[1], l_sem.at[2], partner)

    tz_copy(cls).start()
    pair_copy(h).start()
    for q in range(STEPS):
        z_copy(q, cls).start()
        for d in range(2):
            y_copy(q, d, cls, yo_send).start()
    label_send(k).start()

    total[...] = jnp.zeros_like(total)
    gsum[...] = jnp.zeros_like(gsum)
    lane = lax.broadcasted_iota(jnp.int32, (8, 512), 1)
    wide_row = jnp.broadcast_to(coeff_row, (8, 512))
    diff = wide_row - 2.0 * pltpu.roll(wide_row, 511, 1) + pltpu.roll(wide_row, 510, 1)
    diff = jnp.where(lane < 510, diff, 0.0)
    pen_row[...] = diff - 2.0 * pltpu.roll(diff, 1, 1) + pltpu.roll(diff, 2, 1)

    tz_copy(y * 2 + 1 - h).wait_recv()
    for j in range(1, 4):
        ty_copy(j, y).start()

    def stage_a(q):
        other = y * 2 + 1 - h
        z_copy(q, other).wait_recv()
        for d in range(2):
            y_copy(q, d, other, yz_send).start()
        d_copy(q, y, 1).start()

    def stage_b(q):
        for d, source in ((0, down), (1, up)):
            block = band(q, source * 2 * rows, 2 * rows)
            remote(block, block, yo_send.at[d], y_recv.at[d, q], {"y": (up, down)[d]}).wait_recv()
        op_copy(q, jnp.where(lax.rem(q, 2) == 0, down, up)).start()
        d_copy(q, down, 1).start()
        d_copy(q, up, 1).start()

    def stage_c(q):
        op_copy(q, across).wait_recv()
        d_copy(q, across, 1).start()

    contract = (((1,), (1,)), ((), ()))

    def wait_partner(q):
        theirs = held.at[q, 1 - k]
        remote(theirs, theirs, d_send.at[0], d_recv.at[q], partner).wait_recv()

    def prepare(q):
        both = [jnp.dot(matrix[...].astype(BF16), held[q, core], preferred_element_type=F32) for core in range(2)]
        scores = jnp.concatenate(both, axis=1)
        exponent = jnp.exp(scores - jnp.max(scores, axis=0, keepdims=True))
        probs = exponent / jnp.sum(exponent, axis=0, keepdims=True)
        later_factors[...] = pair_weights(pairs[k], probs)
        lab_rows = [
            labs[core, pl.ds(q * (half // 128) + i, 1), :] for core in range(2) for i in range(half // 128)
        ]
        lab = jnp.concatenate(lab_rows, axis=1)
        one_hot = lax.broadcasted_iota(jnp.int32, (8, 2 * half), 0) == lab
        later_resids[...] = jnp.where(one_hot, 1.0, 0.0) - probs

    def next_chunk():
        factors[...] = later_factors[...]
        resids[...] = later_resids[...]

    def add_products(q, s):
        left, right, extra = None, None, None
        for core in range(2):
            block = held[q, core]
            span = slice(core * half, (core + 1) * half)
            scaled = (block.astype(F32) * factors[s : s + 1, span]).astype(BF16)
            first = lax.dot_general(scaled[:256], block[:256], contract, preferred_element_type=F32)
            second = lax.dot_general(scaled, block[256:], contract, preferred_element_type=F32)
            left = first if left is None else left + first
            right = second if right is None else right + second
            if s == 0:
                resid = resids[:, span].astype(BF16)
                term = lax.dot_general(resid, block, contract, preferred_element_type=F32)
                extra = term if extra is None else extra + term
        total[s, 0:2, :, :, 0:256] += left.reshape(2, 4, 32, 256)
        total[s, :, :, :, 256:512] += right.reshape(4, 4, 32, 256)
        if s == 0:
            gsum[...] += extra

    for t in range(6):
        stage_a(t)
        if t >= 2:
            stage_b(t - 2)
        if t >= 4:
            stage_c(t - 4)
    for j in range(1, 4):
        ty_copy(4 - j, lax.rem(y + 4 - j, 4)).wait_recv()
    pair_copy(1 - h).wait_recv()
    label_send(1 - k).wait_recv()
    for c in range(CLASSES):
        tile = tiles[c]
        matrix[c : c + 1, :] = jnp.concatenate([tile[j : j + 1, :] for j in range(4)], axis=1)
    wait_partner(0)
    prepare(0)
    next_chunk()

    def step(t, carry):
        for stage, first in ((stage_a, 6), (stage_b, 4), (stage_c, 2)):

            @pl.when(t < STEPS - first)
            def _():
                stage(t + first)

        wait_partner(t + 1)
        prepare(t + 1)
        for s in range(5):
            add_products(t, s)
        next_chunk()
        return carry

    lax.fori_loop(0, STEPS - 1, step, 0)

    def turn(s):
        ahead = lax.rem(k + s, 2) == 0
        return jnp.where(ahead, 1, 3), jnp.where(ahead, 3, 1)

    def around(j):
        return lax.rem(x + j, 4)

    def s_copy(s, j, source):
        tile = scales.at[source, s]
        return remote(tile, tile, s_send.at[0], s_recv.at[4 - j, s], {"x": around(j)})

    def relay_copy(s, b):
        to = {"x": around(turn(s)[0])}
        return remote(relay_q.at[s, b], got_relay.at[s, b], q_send.at[0], relay_recv.at[s, b], to)

    def direct_copy(s, b):
        to = {"x": around(turn(s)[1])}
        return remote(direct_q.at[s, b], got_direct.at[s, b], q_send.at[1], direct_recv.at[s, b], to)

    def joint_copy(s, b):
        to = {"x": around(turn(s)[0])}
        return remote(joint_q.at[s, b], got_joint.at[s, b], q_send.at[2], joint_recv.at[s, b], to)

    def g_copy(j, source):
        return remote(grads.at[source], grads.at[source], g_send.at[0], g_recv.at[4 - j], {"x": around(j)})

    def largest_of(block):
        top = jnp.max(jnp.max(jnp.abs(block), axis=0, keepdims=True), axis=1, keepdims=True)
        return jnp.maximum(top, 1e-30)

    def piece(s, j, b):
        return total[s, 2 * b : 2 * b + 2, pl.ds(around(j), 1)].reshape(64, 512)

    def code(block, inverse):
        return jnp.round(block * inverse).astype(jnp.int32).astype(jnp.int16)

    def plain(block):
        return block.astype(jnp.int32).astype(F32)

    def scale_of(j, s):
        return scales[around(j), s, 0:1, 0:1]

    def finish(s):
        add_products(STEPS - 1, s)
        corner = total[s, 0:2, :, :, 256:512].reshape(256, 256)
        total[s, 2:4, :, :, 0:256] = corner.T.reshape(2, 4, 32, 256)

    def first_sums(s):
        finish(s)
        top = largest_of(total[s].reshape(512, 512))
        scales[x, s] = jnp.broadcast_to(top * (1.0 / LEVELS), (8, 128))
        inverse = LEVELS / top
        for b in range(2):
            relay_q[s, b] = code(piece(s, 2, b), inverse)
            if b == 0:
                for j in (1, 3, 2):
                    s_copy(s, j, x).start()
            relay_copy(s, b).start()
        for b in range(2):
            direct_q[s, b] = code(piece(s, turn(s)[1], b), inverse)
            direct_copy(s, b).start()

    def s_wait(s, j):
        tile = scales.at[around(j), s]
        remote(tile, tile, s_send.at[0], s_recv.at[j, s], {"x": around(j)}).wait_recv()

    def joint_sums(s, b):
        ahead, behind = turn(s)
        relay_copy(s, b).wait_recv()
        if b == 0:
            s_wait(s, behind)
        scale, own = scale_of(behind, s), scale_of(0, s)
        value = plain(got_relay[s, b]) * scale + piece(s, ahead, b)
        joint_q[s, b] = code(value, 1.0 / (scale + own))
        joint_copy(s, b).start()

    def owner(i, e):
        return {"zl": lax.rem(zl + i, 4), "zh": k, "core": lax.rem(k + e, 2)}

    def f_copy(s, block, e):
        to = {"zl": block, "zh": k, "core": lax.rem(k + e, 2)}
        return remote(coded.at[s, block, lax.rem(k + e, 2)], far.at[s, z], f_send.at[block, e], f_recv.at[s], to)

    def to_blocks(blocks, act):
        for block in blocks:
            for e in range(2):
                if e:
                    act(block, e)
                else:
                    pl.when((h != k) | (zl != block))(lambda: act(block, 0))

    def fs_copy(i, e):
        src = small.at[lax.rem(zl + i, 4)]
        return remote(src, far_small.at[z], fs_send.at[i, e], fs_recv.at[0], owner(i, e))

    def to_owners(act):
        for i in (2, 1, 3, 0):
            for e in range(2):
                if i or e:
                    act(i, e)
                else:
                    pl.when(h != k)(lambda: act(0, 0))

    def last_sums(s, b):
        ahead, behind = turn(s)
        joint_copy(s, b).wait_recv()
        direct_copy(s, b).wait_recv()
        if b == 0:
            s_wait(s, ahead)
            s_wait(s, 2)
        value = piece(s, 0, b) + plain(got_direct[s, b]) * scale_of(ahead, s)
        value += plain(got_joint[s, b]) * (scale_of(behind, s) + scale_of(2, s))
        top = largest_of(value)
        out = code(value, LEVELS / top)
        for i in range(2):
            for e in range(2):
                first = i * 32 + e * 16
                coded[s, 2 * b + i, e] = out[first : first + 16, :]
        to_blocks((2 * b, 2 * b + 1), lambda block, e: f_copy(s, block, e).start())

        @pl.when((h == k) & (zl // 2 == b))
        def _():
            pltpu.make_async_copy(coded.at[s, zl, k], far.at[s, z], f_recv.at[s]).start()

        return top * (1.0 / LEVELS)

    def b_copy(n, i, e):
        src = b_q.at[n, lax.rem(zl + i, 4), lax.rem(k + e, 2)]
        return remote(src, far_b.at[n, z], b_send.at[n, i, e], b_recv.at[n], owner(i, e))

    def bs_copy(n, i, e):
        return remote(b_scale.at[n], far_bs.at[n, z], bs_send.at[n, i, e], bs_recv.at[n], owner(i, e))

    def bx_copy(n, j, source):
        src = b_sum.at[n, around(j)]
        return remote(src, got_b.at[n, source], bx_send.at[n], bx_recv.at[n, 4 - j], {"x": around(j)})

    def beta_sums(n):
        s = AROUND + n
        finish(s)
        top = largest_of(total[s].reshape(512, 512))
        b_scale[n] = jnp.broadcast_to(top * (1.0 / LEVELS), (8, 128))
        inverse = LEVELS / top
        for i in range(4):
            for c in range(2):
                for p in range(4):
                    b_q[n, i, c, 16 * p : 16 * (p + 1), :] = code(total[s, i, p, 16 * c : 16 * (c + 1), :], inverse)
        to_owners(lambda i, e: b_copy(n, i, e).start())
        to_owners(lambda i, e: bs_copy(n, i, e).start())

        @pl.when(h == k)
        def _():
            pltpu.make_async_copy(b_q.at[n, zl, k], far_b.at[n, z], b_recv.at[n]).start()
            pltpu.make_async_copy(b_scale.at[n], far_bs.at[n, z], bs_recv.at[n]).start()

    def cross_sums(n):
        pltpu.make_async_copy(far_b.at[n], far_b.at[n], b_recv.at[n]).wait()
        pltpu.make_async_copy(far_bs.at[n], far_bs.at[n], bs_recv.at[n]).wait()
        value = jnp.zeros((64, 512), F32)
        for source in range(8):
            value += plain(far_b[n, source]) * far_bs[n, source, 0:1, 0:1]
        b_sum[n] = value.reshape(4, 16, 512)
        for j in (1, 3, 2):
            bx_copy(n, j, x).start()

    scale2 = jnp.zeros((8, 128), F32)
    for act, s, b in ORDER:
        if act == "beta":
            beta_sums(s - AROUND)
        if act == "cross":
            cross_sums(s - AROUND)
        if act == "first":
            first_sums(s)
            if s == 0:
                grads[x] = gsum[...]
                for j in (1, 3, 2):
                    g_copy(j, x).start()
        if act == "joint":
            joint_sums(s, b)
        if act == "last":
            scale2 = jnp.where(row8 == 2 * s + b, last_sums(s, b), scale2)

    for j in (1, 3, 2):
        g_copy(4 - j, around(4 - j)).wait_recv()
    all_grad = grads[0] + grads[1] + grads[2] + grads[3]
    for i in range(4):
        small[i, 0] = all_grad[:, 128 * i : 128 * (i + 1)]
        small[i, 1] = scale2
    to_owners(lambda i, e: fs_copy(i, e).start())
    pl.when(h == k)(lambda: pltpu.make_async_copy(small.at[zl], far_small.at[z], fs_recv.at[0]).start())

    row0 = zl * 128 + x * 32 + k * 16
    ia = lax.broadcasted_iota(jnp.int32, (16, 512), 0) + row0
    ib = lax.broadcasted_iota(jnp.int32, (16, 512), 1)
    pen = jnp.zeros((16, 512), F32)
    taps = (1.0, -2.0, 1.0)
    for m in range(3):
        inside = (ia - m >= 0) & (ia - m <= 509)
        for n in range(3):
            pen += jnp.where(inside & (ib - n == ia - m), taps[m] * taps[n], 0.0)

    pltpu.make_async_copy(far_small, far_small, fs_recv.at[0]).wait()
    summed = far_small[0, 0]
    for source in range(1, 8):
        summed += far_small[source, 0]
    picked = jnp.sum(jnp.where(row8 == cls, summed, 0.0), axis=0, keepdims=True) * (1.0 / 4096.0)
    pen_part = pen_row[:, pl.ds(pl.multiple_of(zl * 128, 128), 128)]
    final = picked - smoothing[cls] * pen_part
    stage[...] = pltpu.roll(final, lax.rem(128 - (x * 32 + k * 16), 128), 1)
    grad_out[...] = stage[0:1, 0:16]
    for s in range(5):
        if s >= AROUND:
            n = s - AROUND
            value = b_sum[n, x]
            for j in (1, 3, 2):
                bx_copy(n, 4 - j, around(j)).wait_recv()
                value += got_b[n, around(j)]
        else:
            pltpu.make_async_copy(far.at[s], far.at[s], f_recv.at[s]).wait()
            value = jnp.zeros((16, 512), F32)
            for source in range(8):
                value += plain(far[s, source]) * far_small[source, 1, pl.ds(2 * s + zl // 2, 1), 0:1]
        smooth = jnp.float32(0.0)
        for j, number in enumerate(DIAGONAL):
            smooth += jnp.where(slots[s] == number, smoothing[j], 0.0)
        hess_out[s] = value * (1.0 / 4096.0) + pen * smooth

    def sent_all(ref, sem):
        pltpu.make_async_copy(ref, ref, sem).wait()

    tz_copy(cls).wait_send()
    pair_copy(h).wait_send()
    label_send(k).wait_send()
    for j in range(1, 4):
        ty_copy(j, y).wait_send()
    sent_all(sent, z_send.at[0])
    for d in range(2):
        sent_all(held.at[0, 0], yo_send.at[d])
        sent_all(held.at[0, 0], yz_send.at[d])
    sent_all(held.at[0], op_send.at[0])
    sent_all(held.at[pl.ds(0, STEPS // 2)], d_send.at[0])
    sent_all(scales.at[pl.ds(0, 3)], s_send.at[0])
    for n in range(5 - AROUND):
        sent_all(got_b.at[n, pl.ds(0, 3)], bx_send.at[n])
        to_owners(lambda i, e: b_copy(n, i, e).wait_send())
        to_owners(lambda i, e: bs_copy(n, i, e).wait_send())
    for i in range(3):
        sent_all(relay_q, q_send.at[i])
    sent_all(grads.at[pl.ds(0, 3)], g_send.at[0])
    to_blocks(range(4), lambda block, e: sent_all(coded.at[:, 0, 0], f_send.at[block, e]))
    to_owners(lambda i, e: fs_copy(i, e).wait_send())


def local(features, labels, coeffs, smoothing, pair_slots):
    vmem = pl.BlockSpec(memory_space=pltpu.VMEM)
    smem = pl.BlockSpec(memory_space=pltpu.SMEM)
    anyspace = pl.BlockSpec(memory_space=pl.ANY)
    dma = pltpu.SemaphoreType.DMA
    half = features.shape[1] // 2 // STEPS
    late = 5 - AROUND
    wide = pltpu.VMEM((8, 2 * half), F32)
    block = pltpu.VMEM((AROUND, 2, 64, 512), jnp.int16)
    hessian, gradient = pl.pallas_call(
        newton_kernel,
        out_shape=(
            pltpu.VMEM((5, 16, 512), F32),
            pltpu.VMEM((1, 16), F32),
        ),
        in_specs=[anyspace, vmem, anyspace, smem, smem],
        out_specs=(vmem, vmem),
        scratch_shapes=[
            pltpu.VMEM((STEPS, 2, 512, half), BF16),
            pltpu.VMEM((STEPS, 64, half), BF16),
            pltpu.VMEM((5, 4, 4, 32, 512), F32),
            pltpu.VMEM((2, 16, 128), jnp.int32),
            pltpu.VMEM((2, 8, 128), jnp.int32),
            pltpu.VMEM((8, 8, 128), F32),
            pltpu.VMEM((8, 512), F32),
            wide, wide, wide, wide,
            pltpu.VMEM((8, 512), F32),
            pltpu.VMEM((4, AROUND, 8, 128), F32),
            block, block, block, block, block, block,
            pltpu.VMEM((4, 8, 512), F32),
            pltpu.VMEM((AROUND, 4, 2, 16, 512), jnp.int16),
            pltpu.VMEM((4, 2, 8, 128), F32),
            pltpu.VMEM((AROUND, 8, 16, 512), jnp.int16),
            pltpu.VMEM((8, 2, 8, 128), F32),
            pltpu.VMEM((late, 4, 2, 64, 512), jnp.int16),
            pltpu.VMEM((late, 8, 128), F32),
            pltpu.VMEM((late, 8, 64, 512), jnp.int16),
            pltpu.VMEM((late, 8, 8, 128), F32),
            pltpu.VMEM((late, 4, 16, 512), F32),
            pltpu.VMEM((late, 4, 16, 512), F32),
            pltpu.VMEM((8, 512), F32),
            pltpu.VMEM((8, 128), F32),
            dma((1,)), dma((1,)), dma((1,)), dma((STEPS,)), dma((2,)), dma((2,)), dma((2, STEPS)),
            dma((1,)), dma((STEPS,)), dma((1,)), dma((STEPS,)),
            dma((2,)), dma((4,)), dma((4,)), dma((2,)), dma((3,)),
            dma((1,)), dma((4, AROUND)), dma((3,)), dma((AROUND, 2)), dma((AROUND, 2)), dma((AROUND, 2)),
            dma((1,)), dma((4,)), dma((4, 2)), dma((AROUND,)), dma((4, 2)), dma((1,)),
            dma((late, 4, 2)), dma((late,)), dma((late, 4, 2)), dma((late,)), dma((late,)), dma((late, 4)),
        ],
        compiler_params=pltpu.CompilerParams(collective_id=0, has_side_effects=True),
        name="newton",
    )(features, coeffs, labels.reshape(32, 128), pair_slots, smoothing)
    return hessian.transpose(1, 0, 2), gradient


def solution(mesh):
    finer = Mesh(mesh.devices.reshape(4, 4, 2, 4, 2), AXES)
    placed = (P(CLS, DP), P(DP), P(CLS, None), P(), P(CLS))
    return jax.shard_map(
        local,
        mesh=finer,
        in_specs=placed,
        out_specs=(P(DP, CLS, None), P(CLS, DP)),
        check_vma=False,
    )
```

```python
import jax
import jax.numpy as jnp
from jax import lax
from jax.experimental import pallas as pl
from jax.experimental.pallas import tpu as pltpu
from jax.sharding import Mesh
from jax.sharding import PartitionSpec as P

CLASSES = 8
PAIRS = CLASSES * (CLASSES + 1) // 2
STARTS = (8, 15, 21, 26, 30, 33, 35)
DIAGONAL = (0, 8, 15, 21, 26, 30, 33, 35)
AXES = ("zl", "x", "core", "y", "zh")
DP = ("zl", "x", "core")
CLS = ("y", "zh")
MESH = pl.DeviceIdType.MESH
STEPS = 8
AROUND = 4
LEVELS = 32767.0
ORDER = (
    ("first", 0, 0), ("first", 1, 0), ("beta", 4, 0), ("joint", 0, 0), ("joint", 0, 1), ("first", 2, 0), ("joint", 1, 0), ("joint", 1, 1), ("first", 3, 0),
    ("last", 0, 0), ("joint", 2, 0), ("last", 0, 1), ("joint", 2, 1), ("last", 1, 0), ("last", 1, 1), ("joint", 3, 0), ("last", 2, 0), ("joint", 3, 1), ("last", 2, 1),
    ("cross", 4, 0), ("last", 3, 0), ("last", 3, 1),
)
F32 = jnp.float32
BF16 = jnp.bfloat16


def place():
    return {name: lax.axis_index(name) for name in AXES}


def remote(src, dst, send, recv, device):
    return pltpu.make_async_remote_copy(
        src_ref=src, dst_ref=dst, send_sem=send, recv_sem=recv, device_id=device, device_id_type=MESH
    )


def pair_weights(slots, probs):
    pair = jnp.minimum(slots, PAIRS - 1)
    first = jnp.zeros_like(pair)
    start = jnp.zeros_like(pair)
    for before, at in zip((0,) + STARTS, STARTS):
        later = pair >= at
        first += jnp.where(later, 1, 0)
        start += jnp.where(later, at - before, 0)
    second = pair - start + first
    live = (slots < PAIRS)[:, :1]
    first, second = first[:, :1], second[:, :1]
    prob_first = jnp.zeros_like(probs)
    prob_second = jnp.zeros_like(probs)
    for k in range(CLASSES):
        row = probs[k : k + 1, :]
        prob_first += jnp.where(first == k, row, 0.0)
        prob_second += jnp.where(second == k, row, 0.0)
    same = jnp.where(first == second, 1.0, 0.0)
    return jnp.where(live, prob_first * (same - prob_second), 0.0)


def newton_kernel(
    feat, coeffs, labels, slots, smoothing,
    hess_out, grad_out,
    held, sent, total, labs, pairs, tiles, matrix, factors, resids, later_factors, later_resids, gsum, scales,
    relay_q, direct_q, joint_q, got_relay, got_direct, got_joint, grads,
    coded, small, far, far_small, b_q, b_scale, far_b, far_bs, b_sum, got_b, pen_row, stage,
    own_sem, away_sem, z_send, z_recv, yo_send, yz_send, y_recv, op_send, op_recv, d_send, d_recv,
    tz_sem, ty_send, ty_recv, p_sem, l_sem, s_send, s_recv, q_send, relay_recv, direct_recv, joint_recv,
    g_send, g_recv, f_send, f_recv, fs_send, fs_recv, b_send, b_recv, bs_send, bs_recv, bx_send, bx_recv,
):
    at = place()
    k, x, y, h, zl = at["core"], at["x"], at["y"], at["zh"], at["zl"]
    z = h * 4 + zl
    cls = y * 2 + h
    half = held.shape[3]
    rows = feat.shape[0]
    kept = feat.shape[1] // 2
    up, down, across = lax.rem(y + 1, 4), lax.rem(y + 3, 4), lax.rem(y + 2, 4)
    antipode, partner = {"zh": 1 - h}, {"core": 1 - k}

    peers = [{"x": lax.rem(x + j, 4)} for j in range(1, 4)] + [{"y": lax.rem(y + j, 4)} for j in range(1, 4)]
    for a in range(2):
        for i in range(4):
            for e in range(2):
                if a or i or e:
                    peers.append({"zl": lax.rem(zl + i, 4), "zh": lax.rem(h + a, 2), "core": lax.rem(k + e, 2)})
    barrier = pltpu.get_barrier_semaphore()
    for device in peers[::-1]:
        pl.semaphore_signal(barrier, inc=1, device_id=device, device_id_type=MESH)

    def band(q, first, size):
        return held.at[q, k, pl.ds(pl.multiple_of(first, 64), size)]

    def columns(side, q):
        return feat.at[:, pl.ds(pl.multiple_of(side * kept + q * half, half), half)]

    for q in range(STEPS):
        pltpu.make_async_copy(columns(1 - h, q), sent.at[q], away_sem.at[0]).start()
        pltpu.make_async_copy(columns(h, q), band(q, cls * rows, rows), own_sem.at[0]).start()
    label_rows = kept // 128
    own_labels = labels.at[pl.ds(pl.multiple_of(h * label_rows, 8), label_rows)]
    label_copy = pltpu.make_async_copy(own_labels, labs.at[k], l_sem.at[0])
    label_copy.start()

    row8 = lax.broadcasted_iota(jnp.int32, (8, 128), 0)
    mine = jnp.full((8, 128), 40, jnp.int32)
    for s in range(5):
        mine = jnp.where(row8 == s, slots[s], mine)
    pairs[h] = mine
    coeff_row = coeffs[...].astype(F32)
    pieces = [coeff_row[:, 128 * j : 128 * (j + 1)] for j in range(4)]
    tiles[cls] = jnp.concatenate(pieces + [jnp.zeros((4, 128), F32)], axis=0)

    pl.semaphore_wait(barrier, len(peers))
    pltpu.make_async_copy(sent, sent, away_sem.at[0]).wait()
    pltpu.make_async_copy(held.at[0, 0], held.at[0, 0], own_sem.at[0]).wait()
    label_copy.wait()

    def z_copy(q, c):
        return remote(sent.at[q], band(q, c * rows, rows), z_send.at[0], z_recv.at[q], antipode)

    def y_copy(q, d, c, send):
        block = band(q, c * rows, rows)
        return remote(block, block, send.at[d], y_recv.at[d, q], {"y": (up, down)[d]})

    def op_copy(q, source):
        block = band(q, source * 2 * rows, 2 * rows)
        to = {"y": jnp.where(lax.rem(q, 2) == 0, up, down)}
        return remote(block, block, op_send.at[0], op_recv.at[q], to)

    def d_copy(q, source, count):
        block = band(q, source * 2 * rows, 2 * rows * count)
        return remote(block, block, d_send.at[0], d_recv.at[q], partner)

    def tz_copy(c):
        return remote(tiles.at[c], tiles.at[c], tz_sem.at[0], tz_sem.at[1], antipode)

    def ty_copy(j, source):
        block = tiles.at[pl.ds(source * 2, 2)]
        return remote(block, block, ty_send.at[j], ty_recv.at[4 - j], {"y": lax.rem(y + j, 4)})

    def pair_copy(side):
        return remote(pairs.at[side], pairs.at[side], p_sem.at[0], p_sem.at[1], antipode)

    def label_send(core):
        return remote(labs.at[core], labs.at[core], l_sem.at[1], l_sem.at[2], partner)

    tz_copy(cls).start()
    pair_copy(h).start()
    for q in range(STEPS):
        z_copy(q, cls).start()
        for d in range(2):
            y_copy(q, d, cls, yo_send).start()
    label_send(k).start()

    total[...] = jnp.zeros_like(total)
    gsum[...] = jnp.zeros_like(gsum)
    lane = lax.broadcasted_iota(jnp.int32, (8, 512), 1)
    wide_row = jnp.broadcast_to(coeff_row, (8, 512))
    diff = wide_row - 2.0 * pltpu.roll(wide_row, 511, 1) + pltpu.roll(wide_row, 510, 1)
    diff = jnp.where(lane < 510, diff, 0.0)
    pen_row[...] = diff - 2.0 * pltpu.roll(diff, 1, 1) + pltpu.roll(diff, 2, 1)

    tz_copy(y * 2 + 1 - h).wait_recv()
    for j in range(1, 4):
        ty_copy(j, y).start()

    def stage_a(q):
        other = y * 2 + 1 - h
        z_copy(q, other).wait_recv()
        for d in range(2):
            y_copy(q, d, other, yz_send).start()
        d_copy(q, y, 1).start()

    def stage_b(q):
        for d, source in ((0, down), (1, up)):
            block = band(q, source * 2 * rows, 2 * rows)
            remote(block, block, yo_send.at[d], y_recv.at[d, q], {"y": (up, down)[d]}).wait_recv()
        op_copy(q, jnp.where(lax.rem(q, 2) == 0, down, up)).start()
        d_copy(q, down, 1).start()
        d_copy(q, up, 1).start()

    def stage_c(q):
        op_copy(q, across).wait_recv()
        d_copy(q, across, 1).start()

    contract = (((1,), (1,)), ((), ()))

    def wait_partner(q):
        theirs = held.at[q, 1 - k]
        remote(theirs, theirs, d_send.at[0], d_recv.at[q], partner).wait_recv()

    def prepare(q):
        both = [jnp.dot(matrix[...].astype(BF16), held[q, core], preferred_element_type=F32) for core in range(2)]
        scores = jnp.concatenate(both, axis=1)
        exponent = jnp.exp(scores - jnp.max(scores, axis=0, keepdims=True))
        probs = exponent / jnp.sum(exponent, axis=0, keepdims=True)
        later_factors[...] = pair_weights(pairs[k], probs)
        lab_rows = [
            labs[core, pl.ds(q * (half // 128) + i, 1), :] for core in range(2) for i in range(half // 128)
        ]
        lab = jnp.concatenate(lab_rows, axis=1)
        one_hot = lax.broadcasted_iota(jnp.int32, (8, 2 * half), 0) == lab
        later_resids[...] = jnp.where(one_hot, 1.0, 0.0) - probs

    def next_chunk():
        factors[...] = later_factors[...]
        resids[...] = later_resids[...]

    def add_products(q, s):
        left, right, extra = None, None, None
        for core in range(2):
            block = held[q, core]
            span = slice(core * half, (core + 1) * half)
            scaled = (block.astype(F32) * factors[s : s + 1, span]).astype(BF16)
            first = lax.dot_general(scaled[:256], block[:256], contract, preferred_element_type=F32)
            second = lax.dot_general(scaled, block[256:], contract, preferred_element_type=F32)
            left = first if left is None else left + first
            right = second if right is None else right + second
            if s == 0:
                resid = resids[:, span].astype(BF16)
                term = lax.dot_general(resid, block, contract, preferred_element_type=F32)
                extra = term if extra is None else extra + term
        total[s, 0:2, :, :, 0:256] += left.reshape(2, 4, 32, 256)
        total[s, :, :, :, 256:512] += right.reshape(4, 4, 32, 256)
        if s == 0:
            gsum[...] += extra

    for t in range(6):
        stage_a(t)
        if t >= 2:
            stage_b(t - 2)
        if t >= 4:
            stage_c(t - 4)
    for j in range(1, 4):
        ty_copy(4 - j, lax.rem(y + 4 - j, 4)).wait_recv()
    pair_copy(1 - h).wait_recv()
    label_send(1 - k).wait_recv()
    for c in range(CLASSES):
        tile = tiles[c]
        matrix[c : c + 1, :] = jnp.concatenate([tile[j : j + 1, :] for j in range(4)], axis=1)
    wait_partner(0)
    prepare(0)
    next_chunk()

    def step(t, carry):
        for stage, first in ((stage_a, 6), (stage_b, 4), (stage_c, 2)):

            @pl.when(t < STEPS - first)
            def _():
                stage(t + first)

        wait_partner(t + 1)
        prepare(t + 1)
        for s in range(5):
            add_products(t, s)
        next_chunk()
        return carry

    lax.fori_loop(0, STEPS - 1, step, 0)

    def turn(s):
        ahead = lax.rem(k + s, 2) == 0
        return jnp.where(ahead, 1, 3), jnp.where(ahead, 3, 1)

    def around(j):
        return lax.rem(x + j, 4)

    def s_copy(s, j, source):
        tile = scales.at[source, s]
        return remote(tile, tile, s_send.at[0], s_recv.at[4 - j, s], {"x": around(j)})

    def relay_copy(s, b):
        to = {"x": around(turn(s)[0])}
        return remote(relay_q.at[s, b], got_relay.at[s, b], q_send.at[0], relay_recv.at[s, b], to)

    def direct_copy(s, b):
        to = {"x": around(turn(s)[1])}
        return remote(direct_q.at[s, b], got_direct.at[s, b], q_send.at[1], direct_recv.at[s, b], to)

    def joint_copy(s, b):
        to = {"x": around(turn(s)[0])}
        return remote(joint_q.at[s, b], got_joint.at[s, b], q_send.at[2], joint_recv.at[s, b], to)

    def g_copy(j, source):
        return remote(grads.at[source], grads.at[source], g_send.at[0], g_recv.at[4 - j], {"x": around(j)})

    def largest_of(block):
        top = jnp.max(jnp.max(jnp.abs(block), axis=0, keepdims=True), axis=1, keepdims=True)
        return jnp.maximum(top, 1e-30)

    def piece(s, j, b):
        return total[s, 2 * b : 2 * b + 2, pl.ds(around(j), 1)].reshape(64, 512)

    def code(block, inverse):
        return jnp.floor(block * inverse + 0.5).astype(jnp.int32).astype(jnp.int16)

    def plain(block):
        return block.astype(jnp.int32).astype(F32)

    def scale_of(j, s):
        return scales[around(j), s, 0:1, 0:1]

    def finish(s):
        add_products(STEPS - 1, s)
        corner = total[s, 0:2, :, :, 256:512].reshape(256, 256)
        total[s, 2:4, :, :, 0:256] = corner.T.reshape(2, 4, 32, 256)

    def first_sums(s):
        finish(s)
        top = largest_of(total[s].reshape(512, 512))
        scales[x, s] = jnp.broadcast_to(top * (1.0 / LEVELS), (8, 128))
        inverse = LEVELS / top
        for b in range(2):
            relay_q[s, b] = code(piece(s, 2, b), inverse)
            if b == 0:
                for j in (1, 3, 2):
                    s_copy(s, j, x).start()
            relay_copy(s, b).start()
        for b in range(2):
            direct_q[s, b] = code(piece(s, turn(s)[1], b), inverse)
            direct_copy(s, b).start()

    def s_wait(s, j):
        tile = scales.at[around(j), s]
        remote(tile, tile, s_send.at[0], s_recv.at[j, s], {"x": around(j)}).wait_recv()

    def joint_sums(s, b):
        ahead, behind = turn(s)
        relay_copy(s, b).wait_recv()
        if b == 0:
            s_wait(s, behind)
        scale, own = scale_of(behind, s), scale_of(0, s)
        value = plain(got_relay[s, b]) * scale + piece(s, ahead, b)
        joint_q[s, b] = code(value, 1.0 / (scale + own))
        joint_copy(s, b).start()

    def owner(i, e):
        return {"zl": lax.rem(zl + i, 4), "zh": k, "core": lax.rem(k + e, 2)}

    def f_copy(s, block, e):
        to = {"zl": block, "zh": k, "core": lax.rem(k + e, 2)}
        return remote(coded.at[s, block, lax.rem(k + e, 2)], far.at[s, z], f_send.at[block, e], f_recv.at[s], to)

    def to_blocks(blocks, act):
        for block in blocks:
            for e in range(2):
                if e:
                    act(block, e)
                else:
                    pl.when((h != k) | (zl != block))(lambda: act(block, 0))

    def fs_copy(i, e):
        src = small.at[lax.rem(zl + i, 4)]
        return remote(src, far_small.at[z], fs_send.at[i, e], fs_recv.at[0], owner(i, e))

    def to_owners(act):
        for i in (2, 1, 3, 0):
            for e in range(2):
                if i or e:
                    act(i, e)
                else:
                    pl.when(h != k)(lambda: act(0, 0))

    def last_sums(s, b):
        ahead, behind = turn(s)
        joint_copy(s, b).wait_recv()
        direct_copy(s, b).wait_recv()
        if b == 0:
            s_wait(s, ahead)
            s_wait(s, 2)
        value = piece(s, 0, b) + plain(got_direct[s, b]) * scale_of(ahead, s)
        value += plain(got_joint[s, b]) * (scale_of(behind, s) + scale_of(2, s))
        top = (scale_of(0, s) + scale_of(1, s) + scale_of(2, s) + scale_of(3, s)) * LEVELS
        out = code(value, LEVELS / top)
        for i in range(2):
            for e in range(2):
                first = i * 32 + e * 16
                coded[s, 2 * b + i, e] = out[first : first + 16, :]
        to_blocks((2 * b, 2 * b + 1), lambda block, e: f_copy(s, block, e).start())

        @pl.when((h == k) & (zl // 2 == b))
        def _():
            pltpu.make_async_copy(coded.at[s, zl, k], far.at[s, z], f_recv.at[s]).start()

        return top * (1.0 / LEVELS)

    def b_copy(n, i, e):
        src = b_q.at[n, lax.rem(zl + i, 4), lax.rem(k + e, 2)]
        return remote(src, far_b.at[n, z], b_send.at[n, i, e], b_recv.at[n], owner(i, e))

    def bs_copy(n, i, e):
        return remote(b_scale.at[n], far_bs.at[n, z], bs_send.at[n, i, e], bs_recv.at[n], owner(i, e))

    def bx_copy(n, j, source):
        src = b_sum.at[n, around(j)]
        return remote(src, got_b.at[n, source], bx_send.at[n], bx_recv.at[n, 4 - j], {"x": around(j)})

    def beta_sums(n):
        s = AROUND + n
        finish(s)
        top = largest_of(total[s].reshape(512, 512))
        b_scale[n] = jnp.broadcast_to(top * (1.0 / LEVELS), (8, 128))
        inverse = LEVELS / top
        for i in range(4):
            for c in range(2):
                for p in range(4):
                    b_q[n, i, c, 16 * p : 16 * (p + 1), :] = code(total[s, i, p, 16 * c : 16 * (c + 1), :], inverse)
        to_owners(lambda i, e: b_copy(n, i, e).start())
        to_owners(lambda i, e: bs_copy(n, i, e).start())

        @pl.when(h == k)
        def _():
            pltpu.make_async_copy(b_q.at[n, zl, k], far_b.at[n, z], b_recv.at[n]).start()
            pltpu.make_async_copy(b_scale.at[n], far_bs.at[n, z], bs_recv.at[n]).start()

    def cross_sums(n):
        pltpu.make_async_copy(far_b.at[n], far_b.at[n], b_recv.at[n]).wait()
        pltpu.make_async_copy(far_bs.at[n], far_bs.at[n], bs_recv.at[n]).wait()
        value = jnp.zeros((64, 512), F32)
        for source in range(8):
            value += plain(far_b[n, source]) * far_bs[n, source, 0:1, 0:1]
        b_sum[n] = value.reshape(4, 16, 512)
        for j in (1, 3, 2):
            bx_copy(n, j, x).start()

    scale2 = jnp.zeros((8, 128), F32)
    for act, s, b in ORDER:
        if act == "beta":
            beta_sums(s - AROUND)
        if act == "cross":
            cross_sums(s - AROUND)
        if act == "first":
            first_sums(s)
            if s == 0:
                grads[x] = gsum[...]
                for j in (1, 3, 2):
                    g_copy(j, x).start()
        if act == "joint":
            joint_sums(s, b)
        if act == "last":
            scale2 = jnp.where(row8 == 2 * s + b, last_sums(s, b), scale2)

    for j in (1, 3, 2):
        g_copy(4 - j, around(4 - j)).wait_recv()
    all_grad = grads[0] + grads[1] + grads[2] + grads[3]
    for i in range(4):
        small[i, 0] = all_grad[:, 128 * i : 128 * (i + 1)]
        small[i, 1] = scale2
    to_owners(lambda i, e: fs_copy(i, e).start())
    pl.when(h == k)(lambda: pltpu.make_async_copy(small.at[zl], far_small.at[z], fs_recv.at[0]).start())

    row0 = zl * 128 + x * 32 + k * 16
    ia = lax.broadcasted_iota(jnp.int32, (16, 512), 0) + row0
    ib = lax.broadcasted_iota(jnp.int32, (16, 512), 1)
    pen = jnp.zeros((16, 512), F32)
    taps = (1.0, -2.0, 1.0)
    for m in range(3):
        inside = (ia - m >= 0) & (ia - m <= 509)
        for n in range(3):
            pen += jnp.where(inside & (ib - n == ia - m), taps[m] * taps[n], 0.0)

    pltpu.make_async_copy(far_small, far_small, fs_recv.at[0]).wait()
    summed = far_small[0, 0]
    for source in range(1, 8):
        summed += far_small[source, 0]
    picked = jnp.sum(jnp.where(row8 == cls, summed, 0.0), axis=0, keepdims=True) * (1.0 / 4096.0)
    pen_part = pen_row[:, pl.ds(pl.multiple_of(zl * 128, 128), 128)]
    final = picked - smoothing[cls] * pen_part
    stage[...] = pltpu.roll(final, lax.rem(128 - (x * 32 + k * 16), 128), 1)
    grad_out[...] = stage[0:1, 0:16]
    for s in range(5):
        if s >= AROUND:
            n = s - AROUND
            value = b_sum[n, x]
            for j in (1, 3, 2):
                bx_copy(n, 4 - j, around(j)).wait_recv()
                value += got_b[n, around(j)]
        else:
            pltpu.make_async_copy(far.at[s], far.at[s], f_recv.at[s]).wait()
            value = jnp.zeros((16, 512), F32)
            for source in range(8):
                value += plain(far[s, source]) * far_small[source, 1, pl.ds(2 * s + zl // 2, 1), 0:1]
        smooth = jnp.float32(0.0)
        for j, number in enumerate(DIAGONAL):
            smooth += jnp.where(slots[s] == number, smoothing[j], 0.0)
        hess_out[s] = value * (1.0 / 4096.0) + pen * smooth

    def sent_all(ref, sem):
        pltpu.make_async_copy(ref, ref, sem).wait()

    tz_copy(cls).wait_send()
    pair_copy(h).wait_send()
    label_send(k).wait_send()
    for j in range(1, 4):
        ty_copy(j, y).wait_send()
    sent_all(sent, z_send.at[0])
    for d in range(2):
        sent_all(held.at[0, 0], yo_send.at[d])
        sent_all(held.at[0, 0], yz_send.at[d])
    sent_all(held.at[0], op_send.at[0])
    sent_all(held.at[pl.ds(0, STEPS // 2)], d_send.at[0])
    sent_all(scales.at[pl.ds(0, 3)], s_send.at[0])
    for n in range(5 - AROUND):
        sent_all(got_b.at[n, pl.ds(0, 3)], bx_send.at[n])
        to_owners(lambda i, e: b_copy(n, i, e).wait_send())
        to_owners(lambda i, e: bs_copy(n, i, e).wait_send())
    for i in range(3):
        sent_all(relay_q, q_send.at[i])
    sent_all(grads.at[pl.ds(0, 3)], g_send.at[0])
    to_blocks(range(4), lambda block, e: sent_all(coded.at[:, 0, 0], f_send.at[block, e]))
    to_owners(lambda i, e: fs_copy(i, e).wait_send())


def local(features, labels, coeffs, smoothing, pair_slots):
    vmem = pl.BlockSpec(memory_space=pltpu.VMEM)
    smem = pl.BlockSpec(memory_space=pltpu.SMEM)
    anyspace = pl.BlockSpec(memory_space=pl.ANY)
    dma = pltpu.SemaphoreType.DMA
    half = features.shape[1] // 2 // STEPS
    late = 5 - AROUND
    wide = pltpu.VMEM((8, 2 * half), F32)
    block = pltpu.VMEM((AROUND, 2, 64, 512), jnp.int16)
    hessian, gradient = pl.pallas_call(
        newton_kernel,
        out_shape=(
            pltpu.VMEM((5, 16, 512), F32),
            pltpu.VMEM((1, 16), F32),
        ),
        in_specs=[anyspace, vmem, anyspace, smem, smem],
        out_specs=(vmem, vmem),
        scratch_shapes=[
            pltpu.VMEM((STEPS, 2, 512, half), BF16),
            pltpu.VMEM((STEPS, 64, half), BF16),
            pltpu.VMEM((5, 4, 4, 32, 512), F32),
            pltpu.VMEM((2, 16, 128), jnp.int32),
            pltpu.VMEM((2, 8, 128), jnp.int32),
            pltpu.VMEM((8, 8, 128), F32),
            pltpu.VMEM((8, 512), F32),
            wide, wide, wide, wide,
            pltpu.VMEM((8, 512), F32),
            pltpu.VMEM((4, AROUND, 8, 128), F32),
            block, block, block, block, block, block,
            pltpu.VMEM((4, 8, 512), F32),
            pltpu.VMEM((AROUND, 4, 2, 16, 512), jnp.int16),
            pltpu.VMEM((4, 2, 8, 128), F32),
            pltpu.VMEM((AROUND, 8, 16, 512), jnp.int16),
            pltpu.VMEM((8, 2, 8, 128), F32),
            pltpu.VMEM((late, 4, 2, 64, 512), jnp.int16),
            pltpu.VMEM((late, 8, 128), F32),
            pltpu.VMEM((late, 8, 64, 512), jnp.int16),
            pltpu.VMEM((late, 8, 8, 128), F32),
            pltpu.VMEM((late, 4, 16, 512), F32),
            pltpu.VMEM((late, 4, 16, 512), F32),
            pltpu.VMEM((8, 512), F32),
            pltpu.VMEM((8, 128), F32),
            dma((1,)), dma((1,)), dma((1,)), dma((STEPS,)), dma((2,)), dma((2,)), dma((2, STEPS)),
            dma((1,)), dma((STEPS,)), dma((1,)), dma((STEPS,)),
            dma((2,)), dma((4,)), dma((4,)), dma((2,)), dma((3,)),
            dma((1,)), dma((4, AROUND)), dma((3,)), dma((AROUND, 2)), dma((AROUND, 2)), dma((AROUND, 2)),
            dma((1,)), dma((4,)), dma((4, 2)), dma((AROUND,)), dma((4, 2)), dma((1,)),
            dma((late, 4, 2)), dma((late,)), dma((late, 4, 2)), dma((late,)), dma((late,)), dma((late, 4)),
        ],
        compiler_params=pltpu.CompilerParams(collective_id=0, has_side_effects=True),
        name="newton",
    )(features, coeffs, labels.reshape(32, 128), pair_slots, smoothing)
    return hessian.transpose(1, 0, 2), gradient


def solution(mesh):
    finer = Mesh(mesh.devices.reshape(4, 4, 2, 4, 2), AXES)
    placed = (P(CLS, DP), P(DP), P(CLS, None), P(), P(CLS))
    return jax.shard_map(
        local,
        mesh=finer,
        in_specs=placed,
        out_specs=(P(DP, CLS, None), P(CLS, DP)),
        check_vma=False,
    )
```
